1024 devices in a mesh: section: 16 (over x_lo, y), replica: 64 (over x_hi, z, core).
Axes of the slice: x: 4 (x_hi: 2, x_lo: 2; x = x_hi * 2 + x_lo), y: 8, z: 16, core: 2. Of those that a mesh axis runs over, the one named last changes fastest.
Arguments:
- gradients: bfloat16 [64, 5120, 1024], P('replica', 'section'), may hold values from -2 to 2
- hidden: bfloat16 [64, 256, 5120], P('replica'), may hold values from -40 to 40
- lengths: int32 [64], P('replica'), may hold values from 64 to 256
- query_weight: bfloat16 [5120, 2560], P(None, 'section'), may hold values from -0.078125 to 0.078125
- master: float32 [16, 64, 5, 1024], P(None, 'replica', None, 'section'), may hold values from -0.078125 to 0.078125
- first_moment: float32 [16, 64, 5, 1024], P(None, 'replica', None, 'section'), may hold values from -3 to 3
- second_moment: float32 [16, 64, 5, 1024], P(None, 'replica', None, 'section'), may hold values from 0.1 to 2
Outputs:
- new_master: float32 [16, 64, 5, 1024], P(None, 'replica', None, 'section')
- new_first: float32 [16, 64, 5, 1024], P(None, 'replica', None, 'section')
- new_second: float32 [16, 64, 5, 1024], P(None, 'replica', None, 'section')
- context: float32 [64, 256, 2560], P('replica', 'section')
The draws below stay inside these ranges and needn't reach their ends.
All inputs are finite; a program needn't handle non-finite values.
Results may differ from the reference program's by a relative error of at most 0.019.
The reference program's roundings to bfloat16 on the way (of `weight`, `projected`, `key_rows`, `queries` and `probs`) count: a program that leaves them out, or rounds other values in their place, can miss the bound.
Values may be sent and summed in bfloat16 or wider, within the bound.
A program may use at most 32 MiB of HBM per device.

```python
import math
import jax
import jax.numpy as jnp
from jax import lax

D = 5120
HEAD = 128
KV_HEADS = 4
SEQ = 256
GROUP = 5
QCOLS = 2560
KCOLS = 512
COLS = 1024
ROW_SLAB = 5
N_SECTION = 16
N_REPLICA = 64


def draw_hidden(key, part):
    base_key = jax.random.fold_in(jax.random.fold_in(key, 11), 0)
    normal_part = jax.random.truncated_normal(base_key, -4.0, 4.0, (N_REPLICA, SEQ, D), jnp.float32)
    return normal_part.astype(jnp.bfloat16)


def with_ends(array, key, least, top_value):
    extent = array.shape
    place = [jax.random.randint(jax.random.fold_in(key, axis), (), 0, extent[axis]) for axis in range(len(extent))]
    array = array.at[tuple(place)].set(least)
    longest = extent.index(max(extent))
    place[longest] = (place[longest] + 1) % extent[longest]
    return array.at[tuple(place)].set(top_value)


def spiked(result, rng, source, target, parts, factor):
    owner, partner = [(jnp.arange(result.shape[dim]) // (result.shape[dim] // parts)).reshape([-1 if axis == dim else 1 for axis in range(result.ndim)]) for dim in (source, target)]
    chosen = jax.random.permutation(rng, parts)[partner]
    strong = (owner == chosen) | (owner == (partner + parts // 2) % parts)
    return jnp.where(strong, factor * result, result)


def levels(key, extent, cuts, smallest, high):
    def one(position, parts):
        heights = jax.random.uniform(jax.random.fold_in(jax.random.fold_in(key, 6), position), (parts,), jnp.float32, smallest / len(cuts), high / len(cuts))
        return jnp.repeat(jnp.exp(heights), extent[position] // parts).reshape((-1,) + (1,) * (len(extent) - position - 1))

    loudness = one(*cuts[0])
    for cut in cuts[1:]:
        loudness = loudness * one(*cut)
    return loudness


def centred(stream_key, shape, scale, most, cuts=(), held_as=jnp.bfloat16):
    loudness = levels(stream_key, shape, cuts, -0.22, 0.18) if cuts else 1.0
    entries = jax.random.normal(stream_key, shape, jnp.float32) * scale * loudness
    return jnp.minimum(jnp.maximum(entries, -most), most).astype(held_as)


def gaussian_with(own_key, shape, spread, most, pieces, heavy, kind=jnp.bfloat16):
    drawn = spread * jax.random.normal(own_key, shape, jnp.float32)
    if pieces:
        drawn = drawn * levels(own_key, shape, pieces, -0.22, 0.18)
    return jnp.clip(spiked(drawn, jax.random.fold_in(own_key, 3), *heavy), -most, most).astype(kind)


def setup_inputs(seed: int = 0) -> dict:
    arg_keys = jax.random.split(jax.random.key(seed), 8)
    gradients = gaussian_with(arg_keys[0], (N_REPLICA, D, COLS), 0.125, 2.0, ((0, 64), (1, 16)), (0, 1, 64, 4.0))
    hidden = draw_hidden(jax.random.fold_in(arg_keys[7], 71), 0)
    lengths = with_ends(jax.random.randint(arg_keys[2], (N_REPLICA,), SEQ // 4, SEQ + 1), jax.random.fold_in(arg_keys[2], 1), SEQ // 4, SEQ).astype(jnp.int32)
    query_weight = centred(arg_keys[3], (D, QCOLS), D ** -0.5, 0.078125, ((1, 16),))
    master = centred(arg_keys[4], (N_SECTION, N_REPLICA, ROW_SLAB, COLS), D ** -0.5, 0.078125, ((1, 64), (3, 16)), jnp.float32)
    first_moment = centred(arg_keys[5], (N_SECTION, N_REPLICA, ROW_SLAB, COLS), 0.5, 3.0, ((1, 64), (3, 16)), jnp.float32)
    second_moment = jnp.clip(jnp.exp(math.log(2.0) - 2.9957323 * jax.random.uniform(arg_keys[6], (N_SECTION, N_REPLICA, ROW_SLAB, COLS), jnp.float32) ** levels(arg_keys[6], (N_SECTION, N_REPLICA, ROW_SLAB, COLS), ((1, 64), (3, 16)), -0.2, 0.2)), 0.1, 2.0)
    return dict(gradients=gradients, hidden=hidden, lengths=lengths, query_weight=query_weight, master=master, first_moment=first_moment, second_moment=second_moment)


BETA_ONE = 0.9
BETA_TWO = 0.95
EPSILON = 1e-08
DECAY = 0.1
RATE = 0.001
CORRECT_ONE = 1.0 - 0.9 ** 50
CORRECT_TWO = 1.0 - 0.95 ** 50

def by_rank(matrix, rank_count):
    row_count = matrix.shape[0]
    key_part = matrix[:, :KCOLS].reshape(row_count, rank_count, KCOLS // rank_count)
    value_part = matrix[:, KCOLS:].reshape(row_count, rank_count, KCOLS // rank_count)
    return jnp.concatenate([key_part, value_part], axis=2).reshape(row_count, COLS)

def adam_step(gradient, weight, first_moment, second_moment):
    new_first = BETA_ONE * first_moment + (1.0 - BETA_ONE) * gradient
    new_second = BETA_TWO * second_moment + (1.0 - BETA_TWO) * gradient * gradient
    direction = new_first / CORRECT_ONE / (jnp.sqrt(new_second / CORRECT_TWO) + EPSILON)
    new_master = weight - RATE * (direction + DECAY * weight)
    return (new_master, new_first, new_second)

def attend(queries, key_rows, value_rows, positions, length):
    query_count = queries.shape[0]
    grouped = queries.reshape(query_count, KV_HEADS, GROUP, HEAD).astype(jnp.float32)
    key_heads = key_rows.reshape(SEQ, KV_HEADS, HEAD).astype(jnp.float32)
    value_heads = value_rows.reshape(SEQ, KV_HEADS, HEAD).astype(jnp.float32)
    scores = jnp.einsum('tkgd,jkd->kgtj', grouped, key_heads) * HEAD ** (-0.5)
    key_pos = jnp.arange(SEQ, dtype=jnp.int32)
    allowed = (key_pos[None, :] <= positions[:, None]) & (key_pos[None, :] < length)
    scores = jnp.where(allowed[None, None], scores, -jnp.inf)
    row_max = lax.optimization_barrier(jnp.max(scores, axis=-1, keepdims=True))
    expo = jnp.exp(scores - row_max)
    probs = (expo / lax.optimization_barrier(jnp.sum(expo, axis=-1, keepdims=True))).astype(jnp.bfloat16)
    mixed = jnp.einsum('kgtj,jkd->tkgd', probs.astype(jnp.float32), value_heads)
    mixed = mixed.reshape(query_count, QCOLS)
    live_rows = positions < length
    return jnp.where(live_rows[:, None], mixed, 0.0).astype(jnp.float32)

def reference(gradients, hidden, lengths, query_weight, master, first_moment, second_moment):

    def add_grad(running, replica_grad):
        return (running + replica_grad.astype(jnp.float32), None)
    summed = lax.scan(add_grad, jnp.zeros((D, COLS), jnp.float32), gradients)[0]
    owned_grad = by_rank(summed, N_SECTION).reshape(N_SECTION, N_REPLICA, D // (N_SECTION * N_REPLICA), COLS)
    new_master, new_first, new_second = adam_step(owned_grad, master, first_moment, second_moment)
    weight = new_master.astype(jnp.bfloat16).reshape(D, COLS)
    kv_width = KCOLS // N_SECTION

    def one_group(operands):
        tokens, length = operands
        projected = jnp.dot(tokens, weight, preferred_element_type=jnp.float32).astype(jnp.bfloat16)
        projected = projected.reshape(SEQ, N_SECTION, COLS // N_SECTION)
        key_rows = projected[:, :, :kv_width].reshape(SEQ, KCOLS)
        value_rows = projected[:, :, kv_width:].reshape(SEQ, KCOLS)
        queries = jnp.dot(tokens, query_weight, preferred_element_type=jnp.float32).astype(jnp.bfloat16)
        return attend(queries, key_rows, value_rows, jnp.arange(SEQ, dtype=jnp.int32), length)
    context = lax.map(one_group, (hidden, lengths))
    return (new_master, new_first, new_second, context)
```

```python
import functools

import jax
import jax.numpy as jnp
from jax import lax
from jax.experimental import pallas as pl
from jax.experimental.pallas import tpu as pltpu
from jax.sharding import PartitionSpec as P

HEAD = 128
KV_HEADS = 4
GROUP = 5
QCOLS = 2560
KCOLS = 512
COLS = 1024
F32 = jnp.float32
BF16 = jnp.bfloat16
MESH = pl.DeviceIdType.MESH

BETA_ONE = 0.9
BETA_TWO = 0.95
EPSILON = 1e-08
DECAY = 0.1
RATE = 0.001
CORRECT_ONE = 1.0 - 0.9**50
CORRECT_TWO = 1.0 - 0.95**50


def adam_step(gradient, weight, first_moment, second_moment):
    new_first = BETA_ONE * first_moment + (1.0 - BETA_ONE) * gradient
    new_second = BETA_TWO * second_moment + (1.0 - BETA_TWO) * gradient * gradient
    direction = new_first / CORRECT_ONE / (jnp.sqrt(new_second / CORRECT_TWO) + EPSILON)
    new_master = weight - RATE * (direction + DECAY * weight)
    return (new_master, new_first, new_second)


def far_first(i):
    half = lax.div(i + 1, 2)
    return 8 + half * (1 - 2 * lax.rem(i, 2))


def near_first(i):
    return far_first(14 - i)


def update_kernel(
    g_hbm, hid_hbm, qw_hbm, ma_hbm, fm_hbm, sm_hbm,
    nm_ref, nf_ref, ns_ref, q_ref, proj_ref,
    gv, hv, qv, ma, fm, sm, ra, xs, rb, z32, zs, rz, sz, ss, rs, m2, agb, w2, w2b,
    lsem, asem_s, asem_r, bsem_s, bsem_r, zsem_s, zsem_r, ssem_s, ssem_r, gz_s, gx_s, gm_s, g_r,
):
    p = lax.axis_index("section")
    r = lax.axis_index("replica")
    core = lax.rem(r, 2)
    z = lax.rem(lax.div(r, 2), 16)
    xh = lax.div(r, 32)
    own_core = lax.div(p, 8)
    mate = r + 1 - 2 * core
    xmate = r + 32 - 64 * xh
    has_self = jnp.where(own_core == core, 1, 0)

    def zdev(zz):
        return xh * 32 + zz * 2 + core

    local = [
        pltpu.make_async_copy(src, dst, lsem.at[i])
        for i, (src, dst) in enumerate(
            ((g_hbm, gv), (hid_hbm, hv), (qw_hbm, qv), (ma_hbm, ma), (fm_hbm, fm), (sm_hbm, sm))
        )
    ]
    for copy in local:
        copy.start()

    barrier = pltpu.get_barrier_semaphore()

    def greet(section, replica):
        pl.semaphore_signal(
            barrier, inc=1, device_id={"section": section, "replica": replica}, device_id_type=MESH
        )

    greet(p, mate)
    greet(p, xmate)

    @pl.loop(0, 15)
    def _(i):
        greet(p, zdev(lax.rem(z + far_first(i), 16)))

    @pl.loop(0, 16)
    def _(i):
        @pl.when(jnp.logical_not(jnp.logical_and(i == p, own_core == core)))
        def _():
            greet(i, r - core + own_core)

    local[1].wait()
    local[2].wait()
    queries = lax.dot_general(hv[...], qv[...], (((1,), (1,)), ((), ())), preferred_element_type=F32)
    q_ref[...] = queries.astype(BF16)
    local[0].wait()
    pl.semaphore_wait(barrier, 33 - has_self)

    def remote(src, dst, send, recv, section, replica):
        return pltpu.make_async_remote_copy(
            src_ref=src, dst_ref=dst, send_sem=send, recv_sem=recv,
            device_id={"section": section, "replica": replica}, device_id_type=MESH,
        )

    theirs = pl.multiple_of((1 - core) * 256, 256)
    mine = pl.multiple_of(core * 256, 256)
    a_copies = [
        remote(gv.at[:, pl.ds(pl.multiple_of(theirs + side * 512, 256), 256)],
               ra.at[:, pl.ds(side * 256, 256)], asem_s.at[side], asem_r.at[side], p, mate)
        for side in range(2)
    ]
    for copy in a_copies:
        copy.start()
    for copy in a_copies:
        copy.wait_recv()

    def paired(row, side):
        own = gv[pl.ds(row, 16), pl.ds(pl.multiple_of(mine + side * 512, 256), 256)]
        return own.astype(F32) + ra[pl.ds(row, 16), pl.ds(side * 256, 256)].astype(F32)

    @pl.loop(0, 10)
    def _(ch):
        row = pl.multiple_of((1 - xh) * 160 + ch * 16, 16)
        for side in range(2):
            xs[pl.ds(pl.multiple_of(ch * 16, 16), 16), side * 256 : side * 256 + 256] = paired(row, side).astype(BF16)

    b_copy = remote(xs, rb, bsem_s, bsem_r, p, xmate)
    b_copy.start()
    b_copy.wait_recv()

    @pl.loop(0, 10)
    def _(ch):
        row = pl.multiple_of(xh * 160 + ch * 16, 16)
        part = pl.multiple_of(ch * 16, 16)
        for side in range(2):
            total = paired(row, side) + rb[pl.ds(part, 16), side * 256 : side * 256 + 256].astype(F32)
            for half in range(2):
                for tile in range(2):
                    z32[pl.ds(ch * 64 + half * 32 + side * 2 + tile, 8, stride=4), :] = total[
                        half * 8 : half * 8 + 8, tile * 128 : tile * 128 + 128
                    ]

    def z_copy(i):
        other = lax.rem(z + far_first(i), 16)
        return remote(zs.at[other], rz.at[z], zsem_s.at[i], zsem_r.at[z], p, zdev(other))

    @pl.loop(0, 15)
    def _(i):
        other = lax.rem(z + far_first(i), 16)
        piece = z32[pl.ds(pl.multiple_of(other * 40, 8), 40), :]
        zs[other] = piece.astype(BF16).reshape(5, 8, 128)
        z_copy(i).start()

    sz[0:40, :] = z32[pl.ds(pl.multiple_of(z * 40, 8), 40), :]
    sz[40:64, :] = jnp.zeros((24, 128), F32)

    @pl.loop(0, 15)
    def _(i):
        other = lax.rem(z + near_first(i), 16)
        remote(zs.at[other], rz.at[other], zsem_s.at[i], zsem_r.at[other], p, zdev(other)).wait_recv()
        sz[0:40, :] += rz[other].astype(F32).reshape(40, 128)

    lane = lax.broadcasted_iota(jnp.int32, (8, 128), 1)
    for cc in range(2):
        for quad in range(2):
            keys = sz[pl.ds(cc * 20 + quad, 8, stride=4), :]
            values = sz[pl.ds(cc * 20 + 2 + quad, 8, stride=4), :]
            for j in range(4):
                key_part = pltpu.roll(keys, (128 - 32 * j) % 128, 1) if j else keys
                value_part = pltpu.roll(values, (160 - 32 * j) % 128, 1) if j != 1 else values
                ss[cc * 8 + quad * 4 + j] = jnp.where(lane < 32, key_part, value_part)

    def s_copy(i):
        section = core * 8 + lax.rem(i, 8)
        return remote(ss.at[i], rs.at[p], ssem_s.at[i], ssem_r.at[p], section, r - core + lax.div(i, 8))

    def s_here(i):
        return jnp.logical_and(core * 8 + lax.rem(i, 8) == p, lax.div(i, 8) == core)

    @pl.loop(0, 16)
    def _(i):
        @pl.when(jnp.logical_not(s_here(i)))
        def _():
            s_copy(i).start()

    @pl.when(own_core == core)
    def _():
        rs[p] = ss[core * 8 + lax.rem(p, 8)]

    for copy in local[3:]:
        copy.wait()

    @pl.loop(0, 16)
    def _(i):
        @pl.when(jnp.logical_not(jnp.logical_and(i == p, own_core == core)))
        def _():
            remote(ss.at[i], rs.at[i], ssem_s.at[i], ssem_r.at[i], i, r - core + own_core).wait_recv()

    @pl.loop(0, 16)
    def _(i):
        rows = pl.ds(i * 5, 5)
        new_master, new_first, new_second = adam_step(
            rs[i, 0:5, 0:64], ma[rows, 0, :], fm[rows, 0, :], sm[rows, 0, :]
        )
        nm_ref[rows, 0, :] = new_master
        nf_ref[rows, 0, :] = new_first
        ns_ref[rows, 0, :] = new_second
        rs[i, 0:5, 0:64] = new_master

    for i in range(8):
        m2[i * 8 : i * 8 + 8, :] = jnp.where(lane < 64, rs[i], pltpu.roll(rs[i + 8], 64, 1))
    for k in range(5):
        agb[r, k] = m2[pl.ds(k, 8, stride=8), :].astype(BF16)

    def gz_copy(i):
        return remote(agb.at[r], agb.at[r], gz_s.at[i], g_r.at[r], p, zdev(lax.rem(z + far_first(i), 16)))

    def gx_copy(i, slot):
        return remote(agb.at[slot], agb.at[slot], gx_s.at[i], g_r.at[slot], p, xmate)

    def gm_copy(i, slot):
        return remote(agb.at[slot], agb.at[slot], gm_s.at[i], g_r.at[slot], p, mate)

    def arrive(slot):
        remote(agb.at[slot], agb.at[slot], gm_s.at[0], g_r.at[slot], p, mate).wait_recv()

    def scatter(slot):
        for k in range(5):
            w2[pl.ds(slot * 5 + k, 8, stride=320), :] = agb[slot, k].astype(F32)

    @pl.loop(0, 15)
    def _(i):
        gz_copy(i).start()

    gx_copy(15, r).start()
    gm_copy(31, r).start()
    scatter(r)

    @pl.loop(0, 15)
    def _(i):
        slot = zdev(lax.rem(z + near_first(i), 16))
        arrive(slot)
        gx_copy(i, slot).start()
        gm_copy(i, slot).start()
        scatter(slot)

    def xslot(i):
        far = jnp.where(i == 0, 0, near_first(i - 1))
        return (1 - xh) * 32 + lax.rem(z + far, 16) * 2 + core

    @pl.loop(0, 16)
    def _(i):
        slot = xslot(i)
        arrive(slot)
        gm_copy(15 + i, slot).start()
        scatter(slot)

    @pl.loop(0, 32)
    def _(i):
        slot = i * 2 + 1 - core
        arrive(slot)
        scatter(slot)

    w2b[...] = w2[...].astype(BF16)
    low = jnp.dot(hv[:, :2560], w2b[...], preferred_element_type=F32)
    high = jnp.dot(hv[:, 2560:], w2b[...], preferred_element_type=F32)
    proj_ref[...] = (low[:, :64] + high[:, 64:]).astype(BF16)

    for copy in a_copies:
        copy.wait_send()
    b_copy.wait_send()

    @pl.loop(0, 15)
    def _(i):
        z_copy(i).wait_send()
        gz_copy(i).wait_send()
        gx_copy(i, zdev(lax.rem(z + near_first(i), 16))).wait_send()
        gm_copy(i, zdev(lax.rem(z + near_first(i), 16))).wait_send()

    gx_copy(15, r).wait_send()
    gm_copy(31, r).wait_send()

    @pl.loop(0, 16)
    def _(i):
        gm_copy(15 + i, xslot(i)).wait_send()

        @pl.when(jnp.logical_not(s_here(i)))
        def _():
            s_copy(i).wait_send()


def update(gradients, tokens, query_weight_t, master, first, second):
    vm = pltpu.VMEM
    dma = pltpu.SemaphoreType.DMA
    state = jax.ShapeDtypeStruct((80, 1, 64), F32)
    anyspace = pl.BlockSpec(memory_space=pl.ANY)
    vmem = pl.BlockSpec(memory_space=pltpu.VMEM)
    return pl.pallas_call(
        update_kernel,
        out_shape=(
            state, state, state,
            jax.ShapeDtypeStruct((256, 160), BF16),
            jax.ShapeDtypeStruct((256, 64), BF16),
        ),
        in_specs=[anyspace] * 6,
        out_specs=(vmem,) * 5,
        scratch_shapes=[
            vm((320, 1024), BF16),
            vm((256, 5120), BF16),
            vm((160, 5120), BF16),
            vm((80, 1, 64), F32), vm((80, 1, 64), F32), vm((80, 1, 64), F32),
            vm((320, 512), BF16),
            vm((160, 512), BF16),
            vm((160, 512), BF16),
            vm((640, 128), F32),
            vm((16, 5, 8, 128), BF16),
            vm((16, 5, 8, 128), BF16),
            vm((64, 128), F32),
            vm((16, 8, 128), F32),
            vm((16, 8, 128), F32),
            vm((64, 128), F32),
            vm((64, 5, 8, 128), BF16),
            vm((2560, 128), F32),
            vm((2560, 128), BF16),
            dma((6,)), dma((2,)), dma((2,)), dma, dma, dma((15,)), dma((16,)),
            dma((16,)), dma((16,)), dma((15,)), dma((16,)), dma((32,)), dma((64,)),
        ],
        compiler_params=pltpu.CompilerParams(collective_id=0, has_side_effects=True),
        name="update",
    )(gradients, tokens, query_weight_t, master, first, second)


def rows_first(arrays, axis, dims):
    turned = [jnp.moveaxis(a, dim, 0) for a, dim in zip(arrays, dims)]
    both = jnp.concatenate([t.reshape(len(t), -1) for t in turned], axis=1)
    filled, at, done = (lax.all_gather(both, axis, axis=0, tiled=True), 0, [])
    for t, dim in zip(turned, dims):
        section = filled[:, at : at + t[0].size].reshape(-1, *t.shape[1:])
        done.append(jnp.moveaxis(section, 0, dim))
        at += t[0].size
    return tuple(done)


def attend(queries, key_rows, value_rows, positions, length):
    query_count = queries.shape[0]
    seq_len = key_rows.shape[0]
    grouped = queries.reshape(query_count, KV_HEADS, GROUP, HEAD)
    key_heads = key_rows.reshape(seq_len, KV_HEADS, HEAD)
    value_heads = value_rows.reshape(seq_len, KV_HEADS, HEAD)
    scores = jnp.einsum(
        "tkgd,jkd->kgtj", grouped, key_heads, preferred_element_type=jnp.float32
    ) * HEAD ** (-0.5)
    key_pos = jnp.arange(seq_len, dtype=jnp.int32)
    allowed = (key_pos[None, :] <= positions[:, None]) & (key_pos[None, :] < length)
    scores = jnp.where(allowed[None, None], scores, -jnp.inf)
    row_max = jnp.max(scores, axis=-1, keepdims=True)
    expo = jnp.exp(scores - row_max)
    probs = (expo / jnp.sum(expo, axis=-1, keepdims=True)).astype(jnp.bfloat16)
    mixed = jnp.einsum("kgtj,jkd->tkgd", probs, value_heads, preferred_element_type=jnp.float32)
    mixed = mixed.reshape(query_count, QCOLS)
    live_rows = positions < length
    return jnp.where(live_rows[:, None], mixed, 0.0)


def on_device(gradients, hidden, lengths, query_weight, master, first_moment, second_moment):
    rank_count = lax.axis_size("section")
    section_index = lax.axis_index("section")
    seq_len = hidden.shape[1]
    states = [a.reshape(80, 1, 64) for a in (master, first_moment, second_moment)]
    new_master, new_first, new_second, query_local, projected = update(
        gradients[0], hidden[0], query_weight.T, *states
    )
    kv_width = KCOLS // rank_count
    queries = lax.all_to_all(query_local, "section", split_axis=0, concat_axis=1, tiled=True)
    key_rows, value_rows = rows_first(
        (projected[:, :kv_width], projected[:, kv_width:]), "section", (1, 1)
    )
    block_rows = seq_len // rank_count
    positions = section_index * block_rows + jnp.arange(block_rows, dtype=jnp.int32)
    context = attend(queries, key_rows, value_rows, positions, lengths[0])
    back = [a.reshape(16, 1, 5, 64) for a in (new_master, new_first, new_second)]
    return (*back, context[None])


def solution(mesh):
    in_specs = (
        P("replica", "section", None),
        P("replica", None, None),
        P("replica"),
        P(None, "section"),
        P(None, "replica", None, "section"),
        P(None, "replica", None, "section"),
        P(None, "replica", None, "section"),
    )
    out_specs = (
        P(None, "replica", None, "section"),
        P(None, "replica", None, "section"),
        P(None, "replica", None, "section"),
        P("replica", "section", None),
    )
    return jax.shard_map(
        on_device, mesh=mesh, in_specs=in_specs, out_specs=out_specs, check_vma=False
    )
```

```python
import functools

import jax
import jax.numpy as jnp
from jax import lax
from jax.experimental import pallas as pl
from jax.experimental.pallas import tpu as pltpu
from jax.sharding import PartitionSpec as P

HEAD = 128
GROUP = 5
QCOLS = 2560
F32 = jnp.float32
BF16 = jnp.bfloat16
MESH = pl.DeviceIdType.MESH

BETA_ONE = 0.9
BETA_TWO = 0.95
EPSILON = 1e-08
DECAY = 0.1
RATE = 0.001
CORRECT_ONE = 1.0 - 0.9**50
CORRECT_TWO = 1.0 - 0.95**50


def adam_step(gradient, weight, first_moment, second_moment):
    new_first = BETA_ONE * first_moment + (1.0 - BETA_ONE) * gradient
    new_second = BETA_TWO * second_moment + (1.0 - BETA_TWO) * gradient * gradient
    direction = new_first / CORRECT_ONE / (jnp.sqrt(new_second / CORRECT_TWO) + EPSILON)
    new_master = weight - RATE * (direction + DECAY * weight)
    return (new_master, new_first, new_second)


def far_first(i):
    half = lax.div(i + 1, 2)
    return 8 + half * (1 - 2 * lax.rem(i, 2))


def near_first(i):
    return far_first(14 - i)


def update_kernel(
    g_hbm, hid_hbm, qw_hbm, ma_hbm, fm_hbm, sm_hbm, len_ref,
    nm_ref, nf_ref, ns_ref, ctx_ref,
    gv, hv, qv, ma, fm, sm, ra, xs, rb, z32, zs, rz, sz, ss, rs, m2, agb, w2, w2b,
    qs, qr, qall, kvs, kvr, keys_all, values_all, cs, cr,
    lsem, asem_s, asem_r, bsem_s, bsem_r, zsem_s, zsem_r, ssem_s, ssem_r, gz_s, gx_s, gm_s, g_r,
    qsem_s, qsem_r, ksem_s, ksem_r, csem_s, csem_r,
):
    p = lax.axis_index("section")
    r = lax.axis_index("replica")
    core = lax.rem(r, 2)
    z = lax.rem(lax.div(r, 2), 16)
    xh = lax.div(r, 32)
    own_core = lax.div(p, 8)
    mate = r + 1 - 2 * core
    xmate = r + 32 - 64 * xh
    has_self = jnp.where(own_core == core, 1, 0)
    kv_head = lax.div(p, 4)
    quarter = lax.rem(p, 4)

    def zdev(zz):
        return xh * 32 + zz * 2 + core

    local = [
        pltpu.make_async_copy(src, dst, lsem.at[i])
        for i, (src, dst) in enumerate(
            ((g_hbm, gv), (hid_hbm, hv), (qw_hbm, qv), (ma_hbm, ma), (fm_hbm, fm), (sm_hbm, sm))
        )
    ]
    for copy in local:
        copy.start()

    barrier = pltpu.get_barrier_semaphore()

    def greet(section, replica):
        pl.semaphore_signal(
            barrier, inc=1, device_id={"section": section, "replica": replica}, device_id_type=MESH
        )

    greet(p, mate)
    greet(p, xmate)

    @pl.loop(0, 15)
    def _(i):
        greet(p, zdev(lax.rem(z + far_first(i), 16)))

    @pl.loop(0, 16)
    def _(i):
        @pl.when(jnp.logical_not(jnp.logical_and(i == p, own_core == core)))
        def _():
            greet(i, r - core + own_core)

    @pl.loop(1, 4)
    def _(i):
        greet(kv_head * 4 + lax.rem(quarter + i, 4), r)
        greet(lax.rem(kv_head + i, 4) * 4 + quarter, r)

    local[1].wait()
    local[2].wait()
    queries = lax.dot_general(hv[...], qv[...], (((1,), (1,)), ((), ())), preferred_element_type=F32)
    queries = queries.astype(BF16)
    for j in range(4):
        for m in range(4):
            qs[j, m * 16 : m * 16 + 16, 0:160] = queries[m * 64 + j * 16 : m * 64 + j * 16 + 16]
    local[0].wait()
    pl.semaphore_wait(barrier, 39 - has_self)

    def remote(src, dst, send, recv, section, replica):
        return pltpu.make_async_remote_copy(
            src_ref=src, dst_ref=dst, send_sem=send, recv_sem=recv,
            device_id={"section": section, "replica": replica}, device_id_type=MESH,
        )

    theirs = pl.multiple_of((1 - core) * 256, 256)
    mine = pl.multiple_of(core * 256, 256)
    a_copies = [
        remote(gv.at[:, pl.ds(pl.multiple_of(theirs + side * 512, 256), 256)],
               ra.at[:, pl.ds(side * 256, 256)], asem_s.at[side], asem_r.at[side], p, mate)
        for side in range(2)
    ]
    for copy in a_copies:
        copy.start()

    def q_copy(i):
        other = lax.rem(quarter + i, 4)
        return remote(qs.at[other], qr.at[quarter], qsem_s.at[i], qsem_r.at[quarter], kv_head * 4 + other, r)

    @pl.loop(1, 4)
    def _(i):
        q_copy(i).start()

    qr[quarter] = qs[quarter]
    for copy in a_copies:
        copy.wait_recv()

    def paired(row, side):
        own = gv[pl.ds(row, 16), pl.ds(pl.multiple_of(mine + side * 512, 256), 256)]
        return own.astype(F32) + ra[pl.ds(row, 16), pl.ds(side * 256, 256)].astype(F32)

    @pl.loop(0, 10)
    def _(ch):
        row = pl.multiple_of((1 - xh) * 160 + ch * 16, 16)
        for side in range(2):
            xs[pl.ds(pl.multiple_of(ch * 16, 16), 16), side * 256 : side * 256 + 256] = paired(row, side).astype(BF16)

    b_copy = remote(xs, rb, bsem_s, bsem_r, p, xmate)
    b_copy.start()
    b_copy.wait_recv()

    @pl.loop(0, 10)
    def _(ch):
        row = pl.multiple_of(xh * 160 + ch * 16, 16)
        part = pl.multiple_of(ch * 16, 16)
        for side in range(2):
            total = paired(row, side) + rb[pl.ds(part, 16), side * 256 : side * 256 + 256].astype(F32)
            for half in range(2):
                for tile in range(2):
                    z32[pl.ds(ch * 64 + half * 32 + side * 2 + tile, 8, stride=4), :] = total[
                        half * 8 : half * 8 + 8, tile * 128 : tile * 128 + 128
                    ]

    def z_copy(i):
        other = lax.rem(z + far_first(i), 16)
        return remote(zs.at[other], rz.at[z], zsem_s.at[i], zsem_r.at[z], p, zdev(other))

    @pl.loop(0, 15)
    def _(i):
        other = lax.rem(z + far_first(i), 16)
        piece = z32[pl.ds(pl.multiple_of(other * 40, 8), 40), :]
        zs[other] = piece.astype(BF16).reshape(5, 8, 128)
        z_copy(i).start()

    @pl.loop(1, 4)
    def _(i):
        other = lax.rem(quarter + i, 4)
        remote(qs.at[other], qr.at[other], qsem_s.at[i], qsem_r.at[other], kv_head * 4 + other, r).wait_recv()

    for j in range(4):
        qall[:, j * 160 : j * 160 + 160] = qr[j, :, 0:160]

    sz[0:40, :] = z32[pl.ds(pl.multiple_of(z * 40, 8), 40), :]
    sz[40:64, :] = jnp.zeros((24, 128), F32)

    @pl.loop(0, 15)
    def _(i):
        other = lax.rem(z + near_first(i), 16)
        remote(zs.at[other], rz.at[other], zsem_s.at[i], zsem_r.at[other], p, zdev(other)).wait_recv()
        sz[0:40, :] += rz[other].astype(F32).reshape(40, 128)

    lane = lax.broadcasted_iota(jnp.int32, (8, 128), 1)
    for cc in range(2):
        for quad in range(2):
            keys = sz[pl.ds(cc * 20 + quad, 8, stride=4), :]
            values = sz[pl.ds(cc * 20 + 2 + quad, 8, stride=4), :]
            for j in range(4):
                key_part = pltpu.roll(keys, (128 - 32 * j) % 128, 1) if j else keys
                value_part = pltpu.roll(values, (160 - 32 * j) % 128, 1) if j != 1 else values
                ss[cc * 8 + quad * 4 + j] = jnp.where(lane < 32, key_part, value_part)

    def s_copy(i):
        section = core * 8 + lax.rem(i, 8)
        return remote(ss.at[i], rs.at[p], ssem_s.at[i], ssem_r.at[p], section, r - core + lax.div(i, 8))

    def s_here(i):
        return jnp.logical_and(core * 8 + lax.rem(i, 8) == p, lax.div(i, 8) == core)

    @pl.loop(0, 16)
    def _(i):
        @pl.when(jnp.logical_not(s_here(i)))
        def _():
            s_copy(i).start()

    @pl.when(own_core == core)
    def _():
        rs[p] = ss[core * 8 + lax.rem(p, 8)]

    for copy in local[3:]:
        copy.wait()

    @pl.loop(0, 16)
    def _(i):
        @pl.when(jnp.logical_not(jnp.logical_and(i == p, own_core == core)))
        def _():
            remote(ss.at[i], rs.at[i], ssem_s.at[i], ssem_r.at[i], i, r - core + own_core).wait_recv()

    @pl.loop(0, 16)
    def _(i):
        rows = pl.ds(i * 5, 5)
        new_master, new_first, new_second = adam_step(
            rs[i, 0:5, 0:64], ma[rows, 0, :], fm[rows, 0, :], sm[rows, 0, :]
        )
        nm_ref[rows, 0, :] = new_master
        nf_ref[rows, 0, :] = new_first
        ns_ref[rows, 0, :] = new_second
        rs[i, 0:5, 0:64] = new_master

    for i in range(8):
        m2[i * 8 : i * 8 + 8, :] = jnp.where(lane < 64, rs[i], pltpu.roll(rs[i + 8], 64, 1))
    for k in range(5):
        agb[r, k] = m2[pl.ds(k, 8, stride=8), :].astype(BF16)

    def gz_copy(i):
        return remote(agb.at[r], agb.at[r], gz_s.at[i], g_r.at[r], p, zdev(lax.rem(z + far_first(i), 16)))

    def gx_copy(i, slot):
        return remote(agb.at[slot], agb.at[slot], gx_s.at[i], g_r.at[slot], p, xmate)

    def gm_copy(i, slot):
        return remote(agb.at[slot], agb.at[slot], gm_s.at[i], g_r.at[slot], p, mate)

    def arrive(slot):
        remote(agb.at[slot], agb.at[slot], gm_s.at[0], g_r.at[slot], p, mate).wait_recv()

    def scatter(slot):
        for k in range(5):
            w2[pl.ds(slot * 5 + k, 8, stride=320), :] = agb[slot, k].astype(F32)

    @pl.loop(0, 15)
    def _(i):
        gz_copy(i).start()

    gx_copy(15, r).start()
    gm_copy(31, r).start()
    scatter(r)

    @pl.loop(0, 15)
    def _(i):
        slot = zdev(lax.rem(z + near_first(i), 16))
        arrive(slot)
        gx_copy(i, slot).start()
        gm_copy(i, slot).start()
        scatter(slot)

    def xslot(i):
        far = jnp.where(i == 0, 0, near_first(i - 1))
        return (1 - xh) * 32 + lax.rem(z + far, 16) * 2 + core

    @pl.loop(0, 16)
    def _(i):
        slot = xslot(i)
        arrive(slot)
        gm_copy(15 + i, slot).start()
        scatter(slot)

    @pl.loop(0, 32)
    def _(i):
        slot = i * 2 + 1 - core
        arrive(slot)
        scatter(slot)

    w2b[...] = w2[...].astype(BF16)
    low = jnp.dot(hv[:, :2560], w2b[...], preferred_element_type=F32)
    high = jnp.dot(hv[:, 2560:], w2b[...], preferred_element_type=F32)
    wide = lax.broadcasted_iota(jnp.int32, (128, 128), 1)
    first = low[:128] + pltpu.roll(high[:128], 64, 1)
    second = pltpu.roll(low[128:], 64, 1) + high[128:]
    both = jnp.where(wide < 64, first, second)
    kvs[...] = pltpu.roll(both, quarter * 32, 1).astype(BF16)

    def k_copy(i):
        return remote(
            kvs, kvr.at[quarter], ksem_s.at[i], ksem_r.at[quarter], kv_head * 4 + lax.rem(quarter + i, 4), r
        )

    @pl.loop(1, 4)
    def _(i):
        k_copy(i).start()

    kvr[quarter] = kvs[...]

    @pl.loop(1, 4)
    def _(i):
        other = lax.rem(quarter + i, 4)
        remote(kvs, kvr.at[other], ksem_s.at[i], ksem_r.at[other], kv_head * 4 + other, r).wait_recv()

    block = lax.div(wide, 32)
    for turn in range(4):
        merged = kvr[(3 - turn) % 4].astype(F32)
        for j in range(4):
            if (j + turn) % 4 != 3:
                merged = jnp.where(block == (j + turn) % 4, kvr[j].astype(F32), merged)
        if turn:
            merged = pltpu.roll(merged, 128 - 32 * turn, 1)
        dest = values_all if turn % 2 else keys_all
        dest[(turn // 2) * 128 : (turn // 2) * 128 + 128, :] = merged.astype(BF16)

    token = lax.broadcasted_iota(jnp.int32, (64, 256), 0)
    position = lax.div(token, 16) * 64 + lax.rem(token, 16) + quarter * 16
    key_pos = lax.broadcasted_iota(jnp.int32, (64, 256), 1)
    length = len_ref[0]
    allowed = jnp.logical_and(key_pos <= position, key_pos < length)
    live = position[:, :128] < length
    for h in range(GROUP):
        scores = lax.dot_general(
            qall[:, h * 128 : h * 128 + 128], keys_all[...], (((1,), (1,)), ((), ())), preferred_element_type=F32
        )
        scores = jnp.where(allowed, scores * HEAD ** (-0.5), -jnp.inf)
        expo = jnp.exp(scores - jnp.max(scores, axis=1, keepdims=True))
        probs = (expo / jnp.sum(expo, axis=1, keepdims=True)).astype(BF16)
        mixed = jnp.dot(probs, values_all[...], preferred_element_type=F32)
        mixed = jnp.where(live, mixed, 0.0).astype(BF16)
        for m in range(4):
            cs[m, :, h * 128 : h * 128 + 128] = mixed[m * 16 : m * 16 + 16]

    def c_copy(i):
        other = lax.rem(kv_head + i, 4)
        return remote(cs.at[other], cr.at[kv_head], csem_s.at[i], csem_r.at[kv_head], other * 4 + quarter, r)

    @pl.loop(1, 4)
    def _(i):
        c_copy(i).start()

    cr[kv_head] = cs[kv_head]

    @pl.loop(1, 4)
    def _(i):
        other = lax.rem(kv_head + i, 4)
        remote(cs.at[other], cr.at[other], csem_s.at[i], csem_r.at[other], other * 4 + quarter, r).wait_recv()

    for m in range(4):
        ctx_ref[:, m * 640 : m * 640 + 640] = cr[m].astype(F32)

    for copy in a_copies:
        copy.wait_send()
    b_copy.wait_send()

    @pl.loop(1, 4)
    def _(i):
        q_copy(i).wait_send()
        k_copy(i).wait_send()
        c_copy(i).wait_send()

    @pl.loop(0, 15)
    def _(i):
        z_copy(i).wait_send()
        gz_copy(i).wait_send()
        gx_copy(i, zdev(lax.rem(z + near_first(i), 16))).wait_send()
        gm_copy(i, zdev(lax.rem(z + near_first(i), 16))).wait_send()

    gx_copy(15, r).wait_send()
    gm_copy(31, r).wait_send()

    @pl.loop(0, 16)
    def _(i):
        gm_copy(15 + i, xslot(i)).wait_send()

        @pl.when(jnp.logical_not(s_here(i)))
        def _():
            s_copy(i).wait_send()


def update(gradients, tokens, query_weight_t, master, first, second, lengths):
    vm = pltpu.VMEM
    dma = pltpu.SemaphoreType.DMA
    state = jax.ShapeDtypeStruct((80, 1, 64), F32)
    anyspace = pl.BlockSpec(memory_space=pl.ANY)
    vmem = pl.BlockSpec(memory_space=pltpu.VMEM)
    return pl.pallas_call(
        update_kernel,
        out_shape=(
            state, state, state,
            jax.ShapeDtypeStruct((16, QCOLS), F32),
        ),
        in_specs=[anyspace] * 6 + [pl.BlockSpec(memory_space=pltpu.SMEM)],
        out_specs=(vmem,) * 4,
        scratch_shapes=[
            vm((320, 1024), BF16),
            vm((256, 5120), BF16),
            vm((160, 5120), BF16),
            vm((80, 1, 64), F32), vm((80, 1, 64), F32), vm((80, 1, 64), F32),
            vm((320, 512), BF16),
            vm((160, 512), BF16),
            vm((160, 512), BF16),
            vm((640, 128), F32),
            vm((16, 5, 8, 128), BF16),
            vm((16, 5, 8, 128), BF16),
            vm((64, 128), F32),
            vm((16, 8, 128), F32),
            vm((16, 8, 128), F32),
            vm((64, 128), F32),
            vm((64, 5, 8, 128), BF16),
            vm((2560, 128), F32),
            vm((2560, 128), BF16),
            vm((4, 64, 256), BF16),
            vm((4, 64, 256), BF16),
            vm((64, 640), BF16),
            vm((128, 128), BF16),
            vm((4, 128, 128), BF16),
            vm((256, 128), BF16),
            vm((256, 128), BF16),
            vm((4, 16, 640), BF16),
            vm((4, 16, 640), BF16),
            dma((6,)), dma((2,)), dma((2,)), dma, dma, dma((15,)), dma((16,)),
            dma((16,)), dma((16,)), dma((15,)), dma((16,)), dma((32,)), dma((64,)),
            dma((4,)), dma((4,)), dma((4,)), dma((4,)), dma((4,)), dma((4,)),
        ],
        compiler_params=pltpu.CompilerParams(collective_id=0, has_side_effects=True),
        name="update",
    )(gradients, tokens, query_weight_t, master, first, second, lengths)


def on_device(gradients, hidden, lengths, query_weight, master, first_moment, second_moment):
    states = [a.reshape(80, 1, 64) for a in (master, first_moment, second_moment)]
    *states, context = update(gradients[0], hidden[0], query_weight.T, *states, lengths)
    return (*[a.reshape(16, 1, 5, 64) for a in states], context[None])


def solution(mesh):
    in_specs = (
        P("replica", "section", None),
        P("replica", None, None),
        P("replica"),
        P(None, "section"),
        P(None, "replica", None, "section"),
        P(None, "replica", None, "section"),
        P(None, "replica", None, "section"),
    )
    out_specs = (
        P(None, "replica", None, "section"),
        P(None, "replica", None, "section"),
        P(None, "replica", None, "section"),
        P("replica", "section", None),
    )
    return jax.shard_map(
        on_device, mesh=mesh, in_specs=in_specs, out_specs=out_specs, check_vma=False
    )
```

```python
import functools

import jax
import jax.numpy as jnp
from jax import lax
from jax.experimental import pallas as pl
from jax.experimental.pallas import tpu as pltpu
from jax.sharding import PartitionSpec as P

HEAD = 128
GROUP = 5
QCOLS = 2560
F32 = jnp.float32
BF16 = jnp.bfloat16
MESH = pl.DeviceIdType.MESH

BETA_ONE = 0.9
BETA_TWO = 0.95
EPSILON = 1e-08
DECAY = 0.1
RATE = 0.001
CORRECT_ONE = 1.0 - 0.9**50
CORRECT_TWO = 1.0 - 0.95**50


def adam_step(gradient, weight, first_moment, second_moment):
    new_first = BETA_ONE * first_moment + (1.0 - BETA_ONE) * gradient
    new_second = BETA_TWO * second_moment + (1.0 - BETA_TWO) * gradient * gradient
    direction = new_first / CORRECT_ONE / (jnp.sqrt(new_second / CORRECT_TWO) + EPSILON)
    new_master = weight - RATE * (direction + DECAY * weight)
    return (new_master, new_first, new_second)


def far_first(i):
    half = lax.div(i + 1, 2)
    return 8 + half * (1 - 2 * lax.rem(i, 2))


def near_first(i):
    return far_first(14 - i)


def update_kernel(
    g_hbm, hid_hbm, qw_hbm, ma_hbm, fm_hbm, sm_hbm, len_ref,
    nm_ref, nf_ref, ns_ref, ctx_ref,
    gv, hv, qv, ma, fm, sm, ra, xo32, xs, xr, z32, zs, rz, sz, ss, rs, m2, agb, w2, w2b,
    qs, qr, qall, kvs, kvr, keys_all, values_all, cs, cr,
    lsem, asem_s, asem_r, xsem_s, xsem_r, zsem_s, zsem_r, ssem_s, ssem_r, gz_s, gx_s, gm_s, g_r,
    qsem_s, qsem_r, ksem_s, ksem_r, csem_s, csem_r,
):
    p = lax.axis_index("section")
    r = lax.axis_index("replica")
    core = lax.rem(r, 2)
    z = lax.rem(lax.div(r, 2), 16)
    xh = lax.div(r, 32)
    own_core = lax.div(p, 8)
    mate = r + 1 - 2 * core
    xmate = r + 32 - 64 * xh
    has_self = jnp.where(own_core == core, 1, 0)
    kv_head = lax.div(p, 4)
    quarter = lax.rem(p, 4)
    served = lax.rem(p + 2, 4)

    def zdev(zz):
        return xh * 32 + zz * 2 + core

    local = [
        pltpu.make_async_copy(src, dst, lsem.at[i])
        for i, (src, dst) in enumerate(
            ((g_hbm, gv), (hid_hbm, hv), (qw_hbm, qv), (ma_hbm, ma), (fm_hbm, fm), (sm_hbm, sm))
        )
    ]
    for copy in local:
        copy.start()

    barrier = pltpu.get_barrier_semaphore()

    def greet(section, replica):
        pl.semaphore_signal(
            barrier, inc=1, device_id={"section": section, "replica": replica}, device_id_type=MESH
        )

    greet(p, mate)
    greet(p, xmate)

    @pl.loop(0, 15)
    def _(i):
        greet(p, zdev(lax.rem(z + far_first(i), 16)))

    @pl.loop(0, 16)
    def _(i):
        @pl.when(jnp.logical_not(jnp.logical_and(i == p, own_core == core)))
        def _():
            greet(i, r - core + own_core)

    @pl.loop(1, 4)
    def _(i):
        greet(kv_head * 4 + lax.rem(quarter + i, 4), r)

    @pl.loop(0, 4)
    def _(i):
        greet(i * 4 + served, r)

    local[0].wait()
    pl.semaphore_wait(barrier, 40 - has_self)

    def remote(src, dst, send, recv, section, replica):
        return pltpu.make_async_remote_copy(
            src_ref=src, dst_ref=dst, send_sem=send, recv_sem=recv,
            device_id={"section": section, "replica": replica}, device_id_type=MESH,
        )

    theirs = pl.multiple_of((1 - core) * 256, 256)
    mine = pl.multiple_of(core * 256, 256)
    a_copies = [
        remote(gv.at[pl.ds(row, 160), pl.ds(pl.multiple_of(theirs + side * 512, 256), 256)],
               ra.at[pl.ds(row, 160), pl.ds(side * 256, 256)],
               asem_s.at[turn * 2 + side], asem_r.at[turn * 2 + side], p, mate)
        for turn, row in enumerate((pl.multiple_of((1 - xh) * 160, 16), pl.multiple_of(xh * 160, 16)))
        for side in range(2)
    ]
    for copy in a_copies:
        copy.start()

    def paired(half, out):
        @pl.loop(0, 10)
        def _(ch):
            row = pl.multiple_of(half * 160 + ch * 16, 16)
            for side in range(2):
                own = gv[pl.ds(row, 16), pl.ds(pl.multiple_of(mine + side * 512, 256), 256)]
                total = own.astype(F32) + ra[pl.ds(row, 16), side * 256 : side * 256 + 256].astype(F32)
                for eight in range(2):
                    for tile in range(2):
                        out[pl.ds(ch * 64 + eight * 32 + side * 2 + tile, 8, stride=4), :] = total[
                            eight * 8 : eight * 8 + 8, tile * 128 : tile * 128 + 128
                        ]

    def place(i):
        return lax.rem(z + far_first(i), 16)

    def rows_of(ref, zz):
        return ref[pl.ds(pl.multiple_of(zz * 40, 8), 40), :]

    def x_copy(i):
        return remote(xs.at[place(i)], xr.at[place(i)], xsem_s.at[i], xsem_r.at[place(i)], p, xmate)

    a_copies[0].wait_recv()
    a_copies[1].wait_recv()
    paired(1 - xh, xo32)

    @pl.loop(0, 16)
    def _(i):
        xs[place(i)] = rows_of(xo32, place(i)).astype(BF16).reshape(5, 8, 128)
        x_copy(i).start()

    a_copies[2].wait_recv()
    a_copies[3].wait_recv()
    paired(xh, z32)

    def z_copy(i):
        return remote(zs.at[place(i)], rz.at[z], zsem_s.at[i], zsem_r.at[z], p, zdev(place(i)))

    @pl.loop(0, 15)
    def _(i):
        x_copy(i).wait_recv()
        piece = rows_of(z32, place(i)) + xr[place(i)].astype(F32).reshape(40, 128)
        zs[place(i)] = piece.astype(BF16).reshape(5, 8, 128)
        z_copy(i).start()

    x_copy(15).wait_recv()
    sz[0:40, :] = rows_of(z32, z) + xr[z].astype(F32).reshape(40, 128)
    sz[40:64, :] = jnp.zeros((24, 128), F32)

    local[1].wait()
    local[2].wait()
    queries = lax.dot_general(hv[...], qv[...], (((1,), (1,)), ((), ())), preferred_element_type=F32)
    queries = queries.astype(BF16)
    for j in range(4):
        for m in range(4):
            qs[j, m * 16 : m * 16 + 16, 0:160] = queries[m * 64 + j * 16 : m * 64 + j * 16 + 16]

    def q_copy(i):
        other = lax.rem(quarter + i, 4)
        return remote(
            qs.at[lax.rem(other + 2, 4)], qr.at[quarter], qsem_s.at[i], qsem_r.at[quarter], kv_head * 4 + other, r
        )

    @pl.loop(1, 4)
    def _(i):
        q_copy(i).start()

    qr[quarter] = qs[served]

    @pl.loop(0, 15)
    def _(i):
        other = lax.rem(z + near_first(i), 16)
        remote(zs.at[other], rz.at[other], zsem_s.at[i], zsem_r.at[other], p, zdev(other)).wait_recv()
        sz[0:40, :] += rz[other].astype(F32).reshape(40, 128)

    lane = lax.broadcasted_iota(jnp.int32, (8, 128), 1)
    for cc in range(2):
        for quad in range(2):
            keys = sz[pl.ds(cc * 20 + quad, 8, stride=4), :]
            values = sz[pl.ds(cc * 20 + 2 + quad, 8, stride=4), :]
            for j in range(4):
                key_part = pltpu.roll(keys, (128 - 32 * j) % 128, 1) if j else keys
                value_part = pltpu.roll(values, (160 - 32 * j) % 128, 1) if j != 1 else values
                ss[cc * 8 + quad * 4 + j] = jnp.where(lane < 32, key_part, value_part)

    def s_copy(i):
        section = core * 8 + lax.rem(i, 8)
        return remote(ss.at[i], rs.at[p], ssem_s.at[i], ssem_r.at[p], section, r - core + lax.div(i, 8))

    def s_here(i):
        return jnp.logical_and(core * 8 + lax.rem(i, 8) == p, lax.div(i, 8) == core)

    @pl.loop(0, 16)
    def _(i):
        @pl.when(jnp.logical_not(s_here(i)))
        def _():
            s_copy(i).start()

    @pl.when(own_core == core)
    def _():
        rs[p] = ss[core * 8 + lax.rem(p, 8)]

    @pl.loop(1, 4)
    def _(i):
        other = lax.rem(quarter + i, 4)
        remote(qs.at[other], qr.at[other], qsem_s.at[i], qsem_r.at[other], kv_head * 4 + other, r).wait_recv()

    for j in range(4):
        qall[:, j * 160 : j * 160 + 160] = qr[j, :, 0:160]

    for copy in local[3:]:
        copy.wait()

    @pl.loop(0, 16)
    def _(i):
        @pl.when(jnp.logical_not(jnp.logical_and(i == p, own_core == core)))
        def _():
            remote(ss.at[i], rs.at[i], ssem_s.at[i], ssem_r.at[i], i, r - core + own_core).wait_recv()

    @pl.loop(0, 16)
    def _(i):
        rows = pl.ds(i * 5, 5)
        new_master, new_first, new_second = adam_step(
            rs[i, 0:5, 0:64], ma[rows, 0, :], fm[rows, 0, :], sm[rows, 0, :]
        )
        nm_ref[rows, 0, :] = new_master
        nf_ref[rows, 0, :] = new_first
        ns_ref[rows, 0, :] = new_second
        rs[i, 0:5, 0:64] = new_master

    for i in range(8):
        m2[i * 8 : i * 8 + 8, :] = jnp.where(lane < 64, rs[i], pltpu.roll(rs[i + 8], 64, 1))
    for k in range(5):
        agb[r, k] = m2[pl.ds(k, 8, stride=8), :].astype(BF16)

    def gz_copy(i):
        return remote(agb.at[r], agb.at[r], gz_s.at[i], g_r.at[r], p, zdev(lax.rem(z + far_first(i), 16)))

    def gx_copy(i, slot):
        return remote(agb.at[slot], agb.at[slot], gx_s.at[i], g_r.at[slot], p, xmate)

    def gm_copy(i, slot):
        return remote(agb.at[slot], agb.at[slot], gm_s.at[i], g_r.at[slot], p, mate)

    def arrive(slot):
        remote(agb.at[slot], agb.at[slot], gm_s.at[0], g_r.at[slot], p, mate).wait_recv()

    def scatter(slot):
        for k in range(5):
            w2[pl.ds(slot * 5 + k, 8, stride=320), :] = agb[slot, k].astype(F32)

    @pl.loop(0, 15)
    def _(i):
        gz_copy(i).start()

    gx_copy(15, r).start()
    gm_copy(31, r).start()
    scatter(r)

    def xslot(i):
        far = jnp.where(i == 0, 0, near_first(i - 1))
        return (1 - xh) * 32 + lax.rem(z + far, 16) * 2 + core

    def from_mate(slot):
        arrive(slot + 1 - 2 * core)
        scatter(slot + 1 - 2 * core)

    @pl.loop(0, 15)
    def _(i):
        slot = zdev(lax.rem(z + near_first(i), 16))
        arrive(slot)
        gx_copy(i, slot).start()
        gm_copy(i, slot).start()
        scatter(slot)
        from_mate(zdev(lax.rem(z + jnp.where(i == 0, 0, near_first(i - 1)), 16)))

    @pl.loop(0, 16)
    def _(i):
        slot = xslot(i)
        arrive(slot)
        gm_copy(15 + i, slot).start()
        scatter(slot)
        from_mate(jnp.where(i == 0, zdev(lax.rem(z + 8, 16)), xslot(i - 1)))

    from_mate(xslot(15))

    w2b[...] = w2[...].astype(BF16)
    low = jnp.dot(hv[:, :2560], w2b[...], preferred_element_type=F32)
    high = jnp.dot(hv[:, 2560:], w2b[...], preferred_element_type=F32)
    wide = lax.broadcasted_iota(jnp.int32, (128, 128), 1)
    first = low[:128] + pltpu.roll(high[:128], 64, 1)
    second = pltpu.roll(low[128:], 64, 1) + high[128:]
    both = jnp.where(wide < 64, first, second)
    kvs[...] = pltpu.roll(both, quarter * 32, 1).astype(BF16)

    def k_copy(i):
        return remote(
            kvs, kvr.at[quarter], ksem_s.at[i], ksem_r.at[quarter], kv_head * 4 + lax.rem(quarter + i, 4), r
        )

    @pl.loop(1, 4)
    def _(i):
        k_copy(i).start()

    kvr[quarter] = kvs[...]

    @pl.loop(1, 4)
    def _(i):
        other = lax.rem(quarter + i, 4)
        remote(kvs, kvr.at[other], ksem_s.at[i], ksem_r.at[other], kv_head * 4 + other, r).wait_recv()

    block = lax.div(wide, 32)
    for turn in range(4):
        merged = kvr[(3 - turn) % 4].astype(F32)
        for j in range(4):
            if (j + turn) % 4 != 3:
                merged = jnp.where(block == (j + turn) % 4, kvr[j].astype(F32), merged)
        if turn:
            merged = pltpu.roll(merged, 128 - 32 * turn, 1)
        dest = values_all if turn % 2 else keys_all
        dest[(turn // 2) * 128 : (turn // 2) * 128 + 128, :] = merged.astype(BF16)

    token = lax.broadcasted_iota(jnp.int32, (64, 256), 0)
    position = lax.div(token, 16) * 64 + lax.rem(token, 16) + served * 16
    key_pos = lax.broadcasted_iota(jnp.int32, (64, 256), 1)
    length = len_ref[0]
    allowed = jnp.logical_and(key_pos <= position, key_pos < length)
    live = position[:, :128] < length
    for h in range(GROUP):
        scores = lax.dot_general(
            qall[:, h * 128 : h * 128 + 128], keys_all[...], (((1,), (1,)), ((), ())), preferred_element_type=F32
        )
        scores = jnp.where(allowed, scores * HEAD ** (-0.5), -jnp.inf)
        expo = jnp.exp(scores - jnp.max(scores, axis=1, keepdims=True))
        probs = (expo / jnp.sum(expo, axis=1, keepdims=True)).astype(BF16)
        mixed = jnp.dot(probs, values_all[...], preferred_element_type=F32)
        mixed = jnp.where(live, mixed, 0.0).astype(BF16)
        for m in range(4):
            cs[m, :, h * 128 : h * 128 + 128] = mixed[m * 16 : m * 16 + 16]

    def c_copy(i):
        other = lax.rem(kv_head + 2 + i, 4)
        return remote(cs.at[other], cr.at[kv_head], csem_s.at[i], csem_r.at[kv_head], other * 4 + served, r)

    @pl.loop(0, 4)
    def _(i):
        c_copy(i).start()

    @pl.loop(0, 4)
    def _(i):
        remote(cs.at[i], cr.at[i], csem_s.at[i], csem_r.at[i], i * 4 + served, r).wait_recv()

    for m in range(4):
        ctx_ref[:, m * 640 : m * 640 + 640] = cr[m].astype(F32)

    for copy in a_copies:
        copy.wait_send()

    @pl.loop(0, 4)
    def _(i):
        c_copy(i).wait_send()

    @pl.loop(1, 4)
    def _(i):
        q_copy(i).wait_send()
        k_copy(i).wait_send()

    @pl.loop(0, 15)
    def _(i):
        z_copy(i).wait_send()
        gz_copy(i).wait_send()
        gx_copy(i, zdev(lax.rem(z + near_first(i), 16))).wait_send()
        gm_copy(i, zdev(lax.rem(z + near_first(i), 16))).wait_send()

    gx_copy(15, r).wait_send()
    gm_copy(31, r).wait_send()

    @pl.loop(0, 16)
    def _(i):
        gm_copy(15 + i, xslot(i)).wait_send()
        x_copy(i).wait_send()

        @pl.when(jnp.logical_not(s_here(i)))
        def _():
            s_copy(i).wait_send()


def update(gradients, tokens, query_weight_t, master, first, second, lengths):
    vm = pltpu.VMEM
    dma = pltpu.SemaphoreType.DMA
    state = jax.ShapeDtypeStruct((80, 1, 64), F32)
    anyspace = pl.BlockSpec(memory_space=pl.ANY)
    vmem = pl.BlockSpec(memory_space=pltpu.VMEM)
    return pl.pallas_call(
        update_kernel,
        out_shape=(
            state, state, state,
            jax.ShapeDtypeStruct((16, QCOLS), F32),
        ),
        in_specs=[anyspace] * 6 + [pl.BlockSpec(memory_space=pltpu.SMEM)],
        out_specs=(vmem,) * 4,
        scratch_shapes=[
            vm((320, 1024), BF16),
            vm((256, 5120), BF16),
            vm((160, 5120), BF16),
            vm((80, 1, 64), F32), vm((80, 1, 64), F32), vm((80, 1, 64), F32),
            vm((320, 512), BF16),
            vm((640, 128), F32),
            vm((16, 5, 8, 128), BF16),
            vm((16, 5, 8, 128), BF16),
            vm((640, 128), F32),
            vm((16, 5, 8, 128), BF16),
            vm((16, 5, 8, 128), BF16),
            vm((64, 128), F32),
            vm((16, 8, 128), F32),
            vm((16, 8, 128), F32),
            vm((64, 128), F32),
            vm((64, 5, 8, 128), BF16),
            vm((2560, 128), F32),
            vm((2560, 128), BF16),
            vm((4, 64, 256), BF16),
            vm((4, 64, 256), BF16),
            vm((64, 640), BF16),
            vm((128, 128), BF16),
            vm((4, 128, 128), BF16),
            vm((256, 128), BF16),
            vm((256, 128), BF16),
            vm((4, 16, 640), BF16),
            vm((4, 16, 640), BF16),
            dma((6,)), dma((4,)), dma((4,)), dma((16,)), dma((16,)), dma((15,)), dma((16,)),
            dma((16,)), dma((16,)), dma((15,)), dma((16,)), dma((32,)), dma((64,)),
            dma((4,)), dma((4,)), dma((4,)), dma((4,)), dma((4,)), dma((4,)),
        ],
        compiler_params=pltpu.CompilerParams(collective_id=0, has_side_effects=True),
        name="update",
    )(gradients, tokens, query_weight_t, master, first, second, lengths)


def finish_kernel(*refs):
    sources, targets, held, came, left = refs[:4], refs[4:8], refs[8:12], refs[12], refs[13]
    for i in range(4):
        pltpu.make_async_copy(sources[i], held[i], came.at[i]).start()
    for i in range(4):
        pltpu.make_async_copy(sources[i], held[i], came.at[i]).wait()
        pltpu.make_async_copy(held[i], targets[i], left.at[i]).start()
    for i in range(4):
        pltpu.make_async_copy(held[i], targets[i], left.at[i]).wait()


def finish(arrays):
    anyspace = pl.BlockSpec(memory_space=pl.ANY)
    return pl.pallas_call(
        finish_kernel,
        out_shape=[jax.ShapeDtypeStruct(a.shape, a.dtype) for a in arrays],
        in_specs=[anyspace] * 4,
        out_specs=[anyspace] * 4,
        scratch_shapes=[pltpu.VMEM(a.shape, a.dtype) for a in arrays] + [pltpu.SemaphoreType.DMA((4,))] * 2,
        name="finish",
    )(*arrays)


def on_device(gradients, hidden, lengths, query_weight, master, first_moment, second_moment):
    states = [a.reshape(80, 1, 64) for a in (master, first_moment, second_moment)]
    *states, context = finish(update(gradients[0], hidden[0], query_weight.T, *states, lengths))
    return (*[a.reshape(16, 1, 5, 64) for a in states], context[None])


def solution(mesh):
    in_specs = (
        P("replica", "section", None),
        P("replica", None, None),
        P("replica"),
        P(None, "section"),
        P(None, "replica", None, "section"),
        P(None, "replica", None, "section"),
        P(None, "replica", None, "section"),
    )
    out_specs = (
        P(None, "replica", None, "section"),
        P(None, "replica", None, "section"),
        P(None, "replica", None, "section"),
        P("replica", "section", None),
    )
    return jax.shard_map(
        on_device, mesh=mesh, in_specs=in_specs, out_specs=out_specs, check_vma=False
    )
```

```python
import functools

import jax
import jax.numpy as jnp
from jax import lax
from jax.experimental import pallas as pl
from jax.experimental.pallas import tpu as pltpu
from jax.sharding import PartitionSpec as P

HEAD = 128
GROUP = 5
QCOLS = 2560
F32 = jnp.float32
BF16 = jnp.bfloat16
MESH = pl.DeviceIdType.MESH

BETA_ONE = 0.9
BETA_TWO = 0.95
EPSILON = 1e-08
DECAY = 0.1
RATE = 0.001
CORRECT_ONE = 1.0 - 0.9**50
CORRECT_TWO = 1.0 - 0.95**50


def adam_step(gradient, weight, first_moment, second_moment):
    new_first = BETA_ONE * first_moment + (1.0 - BETA_ONE) * gradient
    new_second = BETA_TWO * second_moment + (1.0 - BETA_TWO) * gradient * gradient
    direction = new_first / CORRECT_ONE / (jnp.sqrt(new_second / CORRECT_TWO) + EPSILON)
    new_master = weight - RATE * (direction + DECAY * weight)
    return (new_master, new_first, new_second)


def far_first(i):
    half = lax.div(i + 1, 2)
    return 8 + half * (1 - 2 * lax.rem(i, 2))


def near_first(i):
    return far_first(14 - i)


def update_kernel(
    g_hbm, hid_hbm, qw_hbm, ma_hbm, fm_hbm, sm_hbm, len_ref,
    nm_ref, nf_ref, ns_ref, ctx_ref,
    gv, hv, qv, ma, fm, sm, ra, xo32, xs, xr, z32, zs, rz, sz, ss, rs, m2, agb, w2, w2b,
    qs, qr, qall, kvs, kvr, keys_all, values_all, cs, cr,
    lsem, asem_s, asem_r, xsem_s, xsem_r, zsem_s, zsem_r, ssem_s, ssem_r, gz_s, gx_s, gm_s, g_r,
    qsem_s, qsem_r, ksem_s, ksem_r, csem_s, csem_r,
):
    p = lax.axis_index("section")
    r = lax.axis_index("replica")
    core = lax.rem(r, 2)
    z = lax.rem(lax.div(r, 2), 16)
    xh = lax.div(r, 32)
    own_core = lax.div(p, 8)
    mate = r + 1 - 2 * core
    xmate = r + 32 - 64 * xh
    has_self = jnp.where(own_core == core, 1, 0)
    kv_head = lax.div(p, 4)
    quarter = lax.rem(p, 4)
    served = lax.rem(p + 2, 4)

    def zdev(zz):
        return xh * 32 + zz * 2 + core

    local = [
        pltpu.make_async_copy(src, dst, lsem.at[i])
        for i, (src, dst) in enumerate(
            ((g_hbm, gv), (hid_hbm, hv), (qw_hbm, qv), (ma_hbm, ma), (fm_hbm, fm), (sm_hbm, sm))
        )
    ]
    for copy in local:
        copy.start()

    barrier = pltpu.get_barrier_semaphore()

    def greet(section, replica):
        pl.semaphore_signal(
            barrier, inc=1, device_id={"section": section, "replica": replica}, device_id_type=MESH
        )

    greet(p, mate)
    greet(p, xmate)

    @pl.loop(0, 15)
    def _(i):
        greet(p, zdev(lax.rem(z + far_first(i), 16)))

    @pl.loop(0, 16)
    def _(i):
        @pl.when(jnp.logical_not(jnp.logical_and(i == p, own_core == core)))
        def _():
            greet(i, r - core + own_core)

    @pl.loop(1, 4)
    def _(i):
        greet(kv_head * 4 + lax.rem(quarter + i, 4), r)

    @pl.loop(0, 4)
    def _(i):
        greet(i * 4 + served, r)

    local[0].wait()
    pl.semaphore_wait(barrier, 40 - has_self)

    def remote(src, dst, send, recv, section, replica):
        return pltpu.make_async_remote_copy(
            src_ref=src, dst_ref=dst, send_sem=send, recv_sem=recv,
            device_id={"section": section, "replica": replica}, device_id_type=MESH,
        )

    theirs = pl.multiple_of((1 - core) * 256, 256)
    mine = pl.multiple_of(core * 256, 256)
    a_copies = [
        remote(gv.at[pl.ds(row, 160), pl.ds(pl.multiple_of(theirs + side * 512, 256), 256)],
               ra.at[pl.ds(row, 160), pl.ds(side * 256, 256)],
               asem_s.at[turn * 2 + side], asem_r.at[turn * 2 + side], p, mate)
        for turn, row in enumerate((pl.multiple_of((1 - xh) * 160, 16), pl.multiple_of(xh * 160, 16)))
        for side in range(2)
    ]
    for copy in a_copies:
        copy.start()

    def paired(half, out):
        @pl.loop(0, 10)
        def _(ch):
            row = pl.multiple_of(half * 160 + ch * 16, 16)
            for side in range(2):
                own = gv[pl.ds(row, 16), pl.ds(pl.multiple_of(mine + side * 512, 256), 256)]
                total = own.astype(F32) + ra[pl.ds(row, 16), side * 256 : side * 256 + 256].astype(F32)
                for eight in range(2):
                    for tile in range(2):
                        out[pl.ds(ch * 64 + eight * 32 + side * 2 + tile, 8, stride=4), :] = total[
                            eight * 8 : eight * 8 + 8, tile * 128 : tile * 128 + 128
                        ]

    def place(i):
        return lax.rem(z + far_first(i), 16)

    def rows_of(ref, zz):
        return ref[pl.ds(pl.multiple_of(zz * 40, 8), 40), :]

    def x_copy(i):
        return remote(xs.at[place(i)], xr.at[place(i)], xsem_s.at[i], xsem_r.at[place(i)], p, xmate)

    a_copies[0].wait_recv()
    a_copies[1].wait_recv()
    paired(1 - xh, xo32)

    @pl.loop(0, 16)
    def _(i):
        xs[place(i)] = rows_of(xo32, place(i)).astype(BF16).reshape(5, 8, 128)
        x_copy(i).start()

    a_copies[2].wait_recv()
    a_copies[3].wait_recv()
    paired(xh, z32)

    def z_copy(i):
        return remote(zs.at[place(i)], rz.at[z], zsem_s.at[i], zsem_r.at[z], p, zdev(place(i)))

    @pl.loop(0, 15)
    def _(i):
        x_copy(i).wait_recv()
        piece = rows_of(z32, place(i)) + xr[place(i)].astype(F32).reshape(40, 128)
        zs[place(i)] = piece.astype(BF16).reshape(5, 8, 128)
        z_copy(i).start()

    x_copy(15).wait_recv()
    sz[0:40, :] = rows_of(z32, z) + xr[z].astype(F32).reshape(40, 128)
    sz[40:64, :] = jnp.zeros((24, 128), F32)

    local[1].wait()
    local[2].wait()
    queries = lax.dot_general(hv[...], qv[...], (((1,), (1,)), ((), ())), preferred_element_type=F32)
    queries = queries.astype(BF16)
    for j in range(4):
        for m in range(4):
            qs[j, m * 16 : m * 16 + 16, 0:160] = queries[m * 64 + j * 16 : m * 64 + j * 16 + 16]

    def q_copy(i):
        other = lax.rem(quarter + i, 4)
        return remote(
            qs.at[lax.rem(other + 2, 4)], qr.at[quarter], qsem_s.at[i], qsem_r.at[quarter], kv_head * 4 + other, r
        )

    @pl.loop(1, 4)
    def _(i):
        q_copy(i).start()

    qr[quarter] = qs[served]

    @pl.loop(0, 15)
    def _(i):
        other = lax.rem(z + near_first(i), 16)
        remote(zs.at[other], rz.at[other], zsem_s.at[i], zsem_r.at[other], p, zdev(other)).wait_recv()
        sz[0:40, :] += rz[other].astype(F32).reshape(40, 128)

    lane = lax.broadcasted_iota(jnp.int32, (8, 128), 1)
    for cc in range(2):
        for quad in range(2):
            keys = sz[pl.ds(cc * 20 + quad, 8, stride=4), :]
            values = sz[pl.ds(cc * 20 + 2 + quad, 8, stride=4), :]
            for j in range(4):
                key_part = pltpu.roll(keys, (128 - 32 * j) % 128, 1) if j else keys
                value_part = pltpu.roll(values, (160 - 32 * j) % 128, 1) if j != 1 else values
                ss[cc * 8 + quad * 4 + j] = jnp.where(lane < 32, key_part, value_part)

    def s_copy(i):
        section = core * 8 + lax.rem(i, 8)
        return remote(ss.at[i], rs.at[p], ssem_s.at[i], ssem_r.at[p], section, r - core + lax.div(i, 8))

    def s_here(i):
        return jnp.logical_and(core * 8 + lax.rem(i, 8) == p, lax.div(i, 8) == core)

    @pl.loop(0, 16)
    def _(i):
        @pl.when(jnp.logical_not(s_here(i)))
        def _():
            s_copy(i).start()

    @pl.when(own_core == core)
    def _():
        rs[p] = ss[core * 8 + lax.rem(p, 8)]

    @pl.loop(1, 4)
    def _(i):
        other = lax.rem(quarter + i, 4)
        remote(qs.at[other], qr.at[other], qsem_s.at[i], qsem_r.at[other], kv_head * 4 + other, r).wait_recv()

    for j in range(4):
        qall[:, j * 160 : j * 160 + 160] = qr[j, :, 0:160]

    for copy in local[3:]:
        copy.wait()

    @pl.loop(0, 16)
    def _(i):
        @pl.when(jnp.logical_not(jnp.logical_and(i == p, own_core == core)))
        def _():
            remote(ss.at[i], rs.at[i], ssem_s.at[i], ssem_r.at[i], i, r - core + own_core).wait_recv()

    @pl.loop(0, 16)
    def _(i):
        rows = pl.ds(i * 5, 5)
        new_master, new_first, new_second = adam_step(
            rs[i, 0:5, 0:64], ma[rows, 0, :], fm[rows, 0, :], sm[rows, 0, :]
        )
        nm_ref[rows, 0, :] = new_master
        nf_ref[rows, 0, :] = new_first
        ns_ref[rows, 0, :] = new_second
        rs[i, 0:5, 0:64] = new_master

    for i in range(8):
        m2[i * 8 : i * 8 + 8, :] = jnp.where(lane < 64, rs[i], pltpu.roll(rs[i + 8], 64, 1))
    for k in range(5):
        agb[r, k] = m2[pl.ds(k, 8, stride=8), :].astype(BF16)

    def gz_copy(i):
        return remote(agb.at[r], agb.at[r], gz_s.at[i], g_r.at[r], p, zdev(lax.rem(z + near_first(i), 16)))

    def gx_copy(i, slot):
        return remote(agb.at[slot], agb.at[slot], gx_s.at[i], g_r.at[slot], p, xmate)

    def gm_copy(i, slot):
        return remote(agb.at[slot], agb.at[slot], gm_s.at[i], g_r.at[slot], p, mate)

    def arrive(slot):
        remote(agb.at[slot], agb.at[slot], gm_s.at[0], g_r.at[slot], p, mate).wait_recv()

    def scatter(slot):
        for k in range(5):
            w2[pl.ds(slot * 5 + k, 8, stride=320), :] = agb[slot, k].astype(F32)

    gx_copy(15, r).start()

    @pl.loop(0, 15)
    def _(i):
        gz_copy(i).start()

    gm_copy(31, r).start()
    scatter(r)

    def xslot(i):
        far = jnp.where(i == 0, 0, near_first(i - 1))
        return (1 - xh) * 32 + lax.rem(z + far, 16) * 2 + core

    def from_mate(slot):
        arrive(slot + 1 - 2 * core)
        scatter(slot + 1 - 2 * core)

    @pl.loop(0, 15)
    def _(i):
        slot = zdev(lax.rem(z + near_first(i), 16))
        arrive(slot)
        gx_copy(i, slot).start()
        gm_copy(i, slot).start()
        scatter(slot)

    @pl.loop(0, 16)
    def _(i):
        slot = xslot(i)
        arrive(slot)
        gm_copy(15 + i, slot).start()
        scatter(slot)
        from_mate(zdev(lax.rem(z + jnp.where(i == 0, 0, near_first(i - 1)), 16)))

    @pl.loop(0, 16)
    def _(i):
        from_mate(xslot(i))

    w2b[...] = w2[...].astype(BF16)
    low = jnp.dot(hv[:, :2560], w2b[...], preferred_element_type=F32)
    high = jnp.dot(hv[:, 2560:], w2b[...], preferred_element_type=F32)
    wide = lax.broadcasted_iota(jnp.int32, (128, 128), 1)
    first = low[:128] + pltpu.roll(high[:128], 64, 1)
    second = pltpu.roll(low[128:], 64, 1) + high[128:]
    both = jnp.where(wide < 64, first, second)
    kvs[...] = pltpu.roll(both, quarter * 32, 1).astype(BF16)

    def k_copy(i):
        return remote(
            kvs, kvr.at[quarter], ksem_s.at[i], ksem_r.at[quarter], kv_head * 4 + lax.rem(quarter + i, 4), r
        )

    @pl.loop(1, 4)
    def _(i):
        k_copy(i).start()

    kvr[quarter] = kvs[...]

    @pl.loop(1, 4)
    def _(i):
        other = lax.rem(quarter + i, 4)
        remote(kvs, kvr.at[other], ksem_s.at[i], ksem_r.at[other], kv_head * 4 + other, r).wait_recv()

    block = lax.div(wide, 32)
    for turn in range(4):
        merged = kvr[(3 - turn) % 4].astype(F32)
        for j in range(4):
            if (j + turn) % 4 != 3:
                merged = jnp.where(block == (j + turn) % 4, kvr[j].astype(F32), merged)
        if turn:
            merged = pltpu.roll(merged, 128 - 32 * turn, 1)
        dest = values_all if turn % 2 else keys_all
        dest[(turn // 2) * 128 : (turn // 2) * 128 + 128, :] = merged.astype(BF16)

    token = lax.broadcasted_iota(jnp.int32, (64, 256), 0)
    position = lax.div(token, 16) * 64 + lax.rem(token, 16) + served * 16
    key_pos = lax.broadcasted_iota(jnp.int32, (64, 256), 1)
    length = len_ref[0]
    allowed = jnp.logical_and(key_pos <= position, key_pos < length)
    live = position[:, :128] < length
    for h in range(GROUP):
        scores = lax.dot_general(
            qall[:, h * 128 : h * 128 + 128], keys_all[...], (((1,), (1,)), ((), ())), preferred_element_type=F32
        )
        scores = jnp.where(allowed, scores * HEAD ** (-0.5), -jnp.inf)
        expo = jnp.exp(scores - jnp.max(scores, axis=1, keepdims=True))
        probs = (expo / jnp.sum(expo, axis=1, keepdims=True)).astype(BF16)
        mixed = jnp.dot(probs, values_all[...], preferred_element_type=F32)
        mixed = jnp.where(live, mixed, 0.0).astype(BF16)
        for m in range(4):
            cs[m, :, h * 128 : h * 128 + 128] = mixed[m * 16 : m * 16 + 16]

    def c_copy(i):
        other = lax.rem(kv_head + 2 + i, 4)
        return remote(cs.at[other], cr.at[kv_head], csem_s.at[i], csem_r.at[kv_head], other * 4 + served, r)

    @pl.loop(0, 4)
    def _(i):
        c_copy(i).start()

    @pl.loop(0, 4)
    def _(i):
        remote(cs.at[i], cr.at[i], csem_s.at[i], csem_r.at[i], i * 4 + served, r).wait_recv()

    for m in range(4):
        ctx_ref[:, m * 640 : m * 640 + 640] = cr[m].astype(F32)

    for copy in a_copies:
        copy.wait_send()

    @pl.loop(0, 4)
    def _(i):
        c_copy(i).wait_send()

    @pl.loop(1, 4)
    def _(i):
        q_copy(i).wait_send()
        k_copy(i).wait_send()

    @pl.loop(0, 15)
    def _(i):
        z_copy(i).wait_send()
        gz_copy(i).wait_send()
        gx_copy(i, zdev(lax.rem(z + near_first(i), 16))).wait_send()
        gm_copy(i, zdev(lax.rem(z + near_first(i), 16))).wait_send()

    gx_copy(15, r).wait_send()
    gm_copy(31, r).wait_send()

    @pl.loop(0, 16)
    def _(i):
        gm_copy(15 + i, xslot(i)).wait_send()
        x_copy(i).wait_send()

        @pl.when(jnp.logical_not(s_here(i)))
        def _():
            s_copy(i).wait_send()


def update(gradients, tokens, query_weight_t, master, first, second, lengths):
    vm = pltpu.VMEM
    dma = pltpu.SemaphoreType.DMA
    state = jax.ShapeDtypeStruct((80, 1, 64), F32)
    anyspace = pl.BlockSpec(memory_space=pl.ANY)
    vmem = pl.BlockSpec(memory_space=pltpu.VMEM)
    return pl.pallas_call(
        update_kernel,
        out_shape=(
            state, state, state,
            jax.ShapeDtypeStruct((16, QCOLS), F32),
        ),
        in_specs=[anyspace] * 6 + [pl.BlockSpec(memory_space=pltpu.SMEM)],
        out_specs=(vmem,) * 4,
        scratch_shapes=[
            vm((320, 1024), BF16),
            vm((256, 5120), BF16),
            vm((160, 5120), BF16),
            vm((80, 1, 64), F32), vm((80, 1, 64), F32), vm((80, 1, 64), F32),
            vm((320, 512), BF16),
            vm((640, 128), F32),
            vm((16, 5, 8, 128), BF16),
            vm((16, 5, 8, 128), BF16),
            vm((640, 128), F32),
            vm((16, 5, 8, 128), BF16),
            vm((16, 5, 8, 128), BF16),
            vm((64, 128), F32),
            vm((16, 8, 128), F32),
            vm((16, 8, 128), F32),
            vm((64, 128), F32),
            vm((64, 5, 8, 128), BF16),
            vm((2560, 128), F32),
            vm((2560, 128), BF16),
            vm((4, 64, 256), BF16),
            vm((4, 64, 256), BF16),
            vm((64, 640), BF16),
            vm((128, 128), BF16),
            vm((4, 128, 128), BF16),
            vm((256, 128), BF16),
            vm((256, 128), BF16),
            vm((4, 16, 640), BF16),
            vm((4, 16, 640), BF16),
            dma((6,)), dma((4,)), dma((4,)), dma((16,)), dma((16,)), dma((15,)), dma((16,)),
            dma((16,)), dma((16,)), dma((15,)), dma((16,)), dma((32,)), dma((64,)),
            dma((4,)), dma((4,)), dma((4,)), dma((4,)), dma((4,)), dma((4,)),
        ],
        compiler_params=pltpu.CompilerParams(collective_id=0, has_side_effects=True),
        name="update",
    )(gradients, tokens, query_weight_t, master, first, second, lengths)


def finish_kernel(*refs):
    sources, targets, held, came, left = refs[:4], refs[4:8], refs[8:12], refs[12], refs[13]
    for i in range(4):
        pltpu.make_async_copy(sources[i], held[i], came.at[i]).start()
    for i in range(4):
        pltpu.make_async_copy(sources[i], held[i], came.at[i]).wait()
        pltpu.make_async_copy(held[i], targets[i], left.at[i]).start()
    for i in range(4):
        pltpu.make_async_copy(held[i], targets[i], left.at[i]).wait()


def finish(arrays):
    anyspace = pl.BlockSpec(memory_space=pl.ANY)
    return pl.pallas_call(
        finish_kernel,
        out_shape=[jax.ShapeDtypeStruct(a.shape, a.dtype) for a in arrays],
        in_specs=[anyspace] * 4,
        out_specs=[anyspace] * 4,
        scratch_shapes=[pltpu.VMEM(a.shape, a.dtype) for a in arrays] + [pltpu.SemaphoreType.DMA((4,))] * 2,
        name="finish",
    )(*arrays)


def on_device(gradients, hidden, lengths, query_weight, master, first_moment, second_moment):
    states = [a.reshape(80, 1, 64) for a in (master, first_moment, second_moment)]
    *states, context = finish(update(gradients[0], hidden[0], query_weight.T, *states, lengths))
    return (*[a.reshape(16, 1, 5, 64) for a in states], context[None])


def solution(mesh):
    in_specs = (
        P("replica", "section", None),
        P("replica", None, None),
        P("replica"),
        P(None, "section"),
        P(None, "replica", None, "section"),
        P(None, "replica", None, "section"),
        P(None, "replica", None, "section"),
    )
    out_specs = (
        P(None, "replica", None, "section"),
        P(None, "replica", None, "section"),
        P(None, "replica", None, "section"),
        P("replica", "section", None),
    )
    return jax.shard_map(
        on_device, mesh=mesh, in_specs=in_specs, out_specs=out_specs, check_vma=False
    )
```

```python
import functools

import jax
import jax.numpy as jnp
from jax import lax
from jax.experimental import pallas as pl
from jax.experimental.pallas import tpu as pltpu
from jax.sharding import PartitionSpec as P

HEAD = 128
GROUP = 5
QCOLS = 2560
F32 = jnp.float32
BF16 = jnp.bfloat16
MESH = pl.DeviceIdType.MESH

BETA_ONE = 0.9
BETA_TWO = 0.95
EPSILON = 1e-08
DECAY = 0.1
RATE = 0.001
CORRECT_ONE = 1.0 - 0.9**50
CORRECT_TWO = 1.0 - 0.95**50


def adam_step(gradient, weight, first_moment, second_moment):
    new_first = BETA_ONE * first_moment + (1.0 - BETA_ONE) * gradient
    new_second = BETA_TWO * second_moment + (1.0 - BETA_TWO) * gradient * gradient
    direction = new_first / CORRECT_ONE / (jnp.sqrt(new_second / CORRECT_TWO) + EPSILON)
    new_master = weight - RATE * (direction + DECAY * weight)
    return (new_master, new_first, new_second)


def far_first(i):
    half = lax.div(i + 1, 2)
    return 8 + half * (1 - 2 * lax.rem(i, 2))


def near_first(i):
    return far_first(14 - i)


def update_kernel(
    g_hbm, hid_hbm, qw_hbm, ma_hbm, fm_hbm, sm_hbm, len_ref,
    nm_ref, nf_ref, ns_ref, ctx_ref,
    gv, hv, qv, ma, fm, sm, ra, xo32, xs, xr, z32, zs, rz, sz, ss, rs, m2, agb, w2, w2b,
    qs, qr, qall, kvs, kvr, keys_all, values_all, cs, cr,
    lsem, asem_s, asem_r, xsem_s, xsem_r, zsem_s, zsem_r, ssem_s, ssem_r, gz_s, gr_s, gx_s, gm_s, g_r,
    qsem_s, qsem_r, ksem_s, ksem_r, csem_s, csem_r,
):
    p = lax.axis_index("section")
    r = lax.axis_index("replica")
    core = lax.rem(r, 2)
    z = lax.rem(lax.div(r, 2), 16)
    xh = lax.div(r, 32)
    own_core = lax.div(p, 8)
    mate = r + 1 - 2 * core
    xmate = r + 32 - 64 * xh
    has_self = jnp.where(own_core == core, 1, 0)
    kv_head = lax.div(p, 4)
    quarter = lax.rem(p, 4)
    served = lax.rem(p + 2, 4)

    def zdev(zz):
        return xh * 32 + zz * 2 + core

    local = [
        pltpu.make_async_copy(src, dst, lsem.at[i])
        for i, (src, dst) in enumerate(
            ((g_hbm, gv), (hid_hbm, hv), (qw_hbm, qv), (ma_hbm, ma), (fm_hbm, fm), (sm_hbm, sm))
        )
    ]
    for copy in local:
        copy.start()

    barrier = pltpu.get_barrier_semaphore()

    def greet(section, replica):
        pl.semaphore_signal(
            barrier, inc=1, device_id={"section": section, "replica": replica}, device_id_type=MESH
        )

    greet(p, mate)
    greet(p, xmate)

    @pl.loop(0, 15)
    def _(i):
        greet(p, zdev(lax.rem(z + far_first(i), 16)))

    @pl.loop(0, 16)
    def _(i):
        @pl.when(jnp.logical_not(jnp.logical_and(i == p, own_core == core)))
        def _():
            greet(i, r - core + own_core)

    @pl.loop(1, 4)
    def _(i):
        greet(kv_head * 4 + lax.rem(quarter + i, 4), r)

    @pl.loop(0, 4)
    def _(i):
        greet(i * 4 + served, r)

    local[0].wait()
    pl.semaphore_wait(barrier, 40 - has_self)

    def remote(src, dst, send, recv, section, replica):
        return pltpu.make_async_remote_copy(
            src_ref=src, dst_ref=dst, send_sem=send, recv_sem=recv,
            device_id={"section": section, "replica": replica}, device_id_type=MESH,
        )

    theirs = pl.multiple_of((1 - core) * 256, 256)
    mine = pl.multiple_of(core * 256, 256)
    a_copies = [
        remote(gv.at[pl.ds(row, 160), pl.ds(pl.multiple_of(theirs + side * 512, 256), 256)],
               ra.at[pl.ds(row, 160), pl.ds(side * 256, 256)],
               asem_s.at[turn * 2 + side], asem_r.at[turn * 2 + side], p, mate)
        for turn, row in enumerate((pl.multiple_of((1 - xh) * 160, 16), pl.multiple_of(xh * 160, 16)))
        for side in range(2)
    ]
    for copy in a_copies:
        copy.start()

    def paired(half, out):
        @pl.loop(0, 10)
        def _(ch):
            row = pl.multiple_of(half * 160 + ch * 16, 16)
            for side in range(2):
                own = gv[pl.ds(row, 16), pl.ds(pl.multiple_of(mine + side * 512, 256), 256)]
                total = own.astype(F32) + ra[pl.ds(row, 16), side * 256 : side * 256 + 256].astype(F32)
                for eight in range(2):
                    for tile in range(2):
                        out[pl.ds(ch * 64 + eight * 32 + side * 2 + tile, 8, stride=4), :] = total[
                            eight * 8 : eight * 8 + 8, tile * 128 : tile * 128 + 128
                        ]

    def place(i):
        return lax.rem(z + far_first(i), 16)

    def rows_of(ref, zz):
        return ref[pl.ds(pl.multiple_of(zz * 40, 8), 40), :]

    def x_copy(i):
        return remote(xs.at[place(i)], xr.at[place(i)], xsem_s.at[i], xsem_r.at[place(i)], p, xmate)

    a_copies[0].wait_recv()
    a_copies[1].wait_recv()
    paired(1 - xh, xo32)

    @pl.loop(0, 16)
    def _(i):
        xs[place(i)] = rows_of(xo32, place(i)).astype(BF16).reshape(5, 8, 128)
        x_copy(i).start()

    a_copies[2].wait_recv()
    a_copies[3].wait_recv()
    paired(xh, z32)

    def z_copy(i):
        return remote(zs.at[place(i)], rz.at[z], zsem_s.at[i], zsem_r.at[z], p, zdev(place(i)))

    @pl.loop(0, 15)
    def _(i):
        x_copy(i).wait_recv()
        piece = rows_of(z32, place(i)) + xr[place(i)].astype(F32).reshape(40, 128)
        zs[place(i)] = piece.astype(BF16).reshape(5, 8, 128)
        z_copy(i).start()

    x_copy(15).wait_recv()
    sz[0:40, :] = rows_of(z32, z) + xr[z].astype(F32).reshape(40, 128)
    sz[40:64, :] = jnp.zeros((24, 128), F32)

    local[1].wait()
    local[2].wait()
    queries = lax.dot_general(hv[...], qv[...], (((1,), (1,)), ((), ())), preferred_element_type=F32)
    queries = queries.astype(BF16)
    for j in range(4):
        for m in range(4):
            qs[j, m * 16 : m * 16 + 16, 0:160] = queries[m * 64 + j * 16 : m * 64 + j * 16 + 16]

    def q_copy(i):
        other = lax.rem(quarter + i, 4)
        return remote(
            qs.at[lax.rem(other + 2, 4)], qr.at[quarter], qsem_s.at[i], qsem_r.at[quarter], kv_head * 4 + other, r
        )

    @pl.loop(1, 4)
    def _(i):
        q_copy(i).start()

    qr[quarter] = qs[served]

    @pl.loop(0, 15)
    def _(i):
        other = lax.rem(z + near_first(i), 16)
        remote(zs.at[other], rz.at[other], zsem_s.at[i], zsem_r.at[other], p, zdev(other)).wait_recv()
        sz[0:40, :] += rz[other].astype(F32).reshape(40, 128)

    lane = lax.broadcasted_iota(jnp.int32, (8, 128), 1)
    for cc in range(2):
        for quad in range(2):
            keys = sz[pl.ds(cc * 20 + quad, 8, stride=4), :]
            values = sz[pl.ds(cc * 20 + 2 + quad, 8, stride=4), :]
            for j in range(4):
                key_part = pltpu.roll(keys, (128 - 32 * j) % 128, 1) if j else keys
                value_part = pltpu.roll(values, (160 - 32 * j) % 128, 1) if j != 1 else values
                ss[cc * 8 + quad * 4 + j] = jnp.where(lane < 32, key_part, value_part)

    def s_copy(i):
        section = core * 8 + lax.rem(i, 8)
        return remote(ss.at[i], rs.at[p], ssem_s.at[i], ssem_r.at[p], section, r - core + lax.div(i, 8))

    def s_here(i):
        return jnp.logical_and(core * 8 + lax.rem(i, 8) == p, lax.div(i, 8) == core)

    @pl.loop(0, 16)
    def _(i):
        @pl.when(jnp.logical_not(s_here(i)))
        def _():
            s_copy(i).start()

    @pl.when(own_core == core)
    def _():
        rs[p] = ss[core * 8 + lax.rem(p, 8)]

    @pl.loop(1, 4)
    def _(i):
        other = lax.rem(quarter + i, 4)
        remote(qs.at[other], qr.at[other], qsem_s.at[i], qsem_r.at[other], kv_head * 4 + other, r).wait_recv()

    for j in range(4):
        qall[:, j * 160 : j * 160 + 160] = qr[j, :, 0:160]

    for copy in local[3:]:
        copy.wait()

    @pl.loop(0, 16)
    def _(i):
        @pl.when(jnp.logical_not(jnp.logical_and(i == p, own_core == core)))
        def _():
            remote(ss.at[i], rs.at[i], ssem_s.at[i], ssem_r.at[i], i, r - core + own_core).wait_recv()

    @pl.loop(0, 16)
    def _(i):
        rows = pl.ds(i * 5, 5)
        new_master, new_first, new_second = adam_step(
            rs[i, 0:5, 0:64], ma[rows, 0, :], fm[rows, 0, :], sm[rows, 0, :]
        )
        nm_ref[rows, 0, :] = new_master
        nf_ref[rows, 0, :] = new_first
        ns_ref[rows, 0, :] = new_second
        rs[i, 0:5, 0:64] = new_master

    for i in range(8):
        m2[i * 8 : i * 8 + 8, :] = jnp.where(lane < 64, rs[i], pltpu.roll(rs[i + 8], 64, 1))
    for k in range(5):
        agb[r, k] = m2[pl.ds(k, 8, stride=8), :].astype(BF16)

    def came(i):
        index = jnp.where(i < 4, i, jnp.where(i < 6, i + 4, jnp.where(i < 10, i - 2, i)))
        return lax.rem(z + near_first(index), 16)

    def gz_copy(i):
        away = (5, 11, 8, 1, 15, 2, 14)[i]
        return remote(agb.at[r], agb.at[r], gz_s.at[i], g_r.at[r], p, zdev(lax.rem(z + away, 16)))

    def gr_copy(i, turn, slot):
        to = zdev(lax.rem(z + (1, 15, 2, 14)[turn], 16))
        return remote(agb.at[slot], agb.at[slot], gr_s.at[(i - 4) * 4 + turn], g_r.at[slot], p, to)

    def gx_copy(i, slot):
        return remote(agb.at[slot], agb.at[slot], gx_s.at[i], g_r.at[slot], p, xmate)

    def gm_copy(i, slot):
        return remote(agb.at[slot], agb.at[slot], gm_s.at[i], g_r.at[slot], p, mate)

    def arrive(slot):
        remote(agb.at[slot], agb.at[slot], gm_s.at[0], g_r.at[slot], p, mate).wait_recv()

    def scatter(slot):
        for k in range(5):
            w2[pl.ds(slot * 5 + k, 8, stride=320), :] = agb[slot, k].astype(F32)

    gx_copy(15, r).start()

    for i in range(7):
        gz_copy(i).start()
    gm_copy(31, r).start()
    scatter(r)

    def xslot(i):
        return (1 - xh) * 32 + jnp.where(i == 0, z, came(i - 1)) * 2 + core

    def from_mate(slot):
        arrive(slot + 1 - 2 * core)
        scatter(slot + 1 - 2 * core)

    @pl.loop(0, 15)
    def _(i):
        slot = zdev(came(i))
        arrive(slot)

        @pl.when(jnp.logical_and(i >= 4, i < 6))
        def _():
            for turn in range(4):
                gr_copy(i, turn, slot).start()

        gx_copy(i, slot).start()
        gm_copy(i, slot).start()
        scatter(slot)

    @pl.loop(0, 16)
    def _(i):
        slot = xslot(i)
        arrive(slot)
        gm_copy(15 + i, slot).start()
        scatter(slot)
        from_mate(zdev(jnp.where(i == 0, z, came(i - 1))))

    @pl.loop(0, 16)
    def _(i):
        from_mate(xslot(i))

    w2b[...] = w2[...].astype(BF16)
    low = jnp.dot(hv[:, :2560], w2b[...], preferred_element_type=F32)
    high = jnp.dot(hv[:, 2560:], w2b[...], preferred_element_type=F32)
    wide = lax.broadcasted_iota(jnp.int32, (128, 128), 1)
    first = low[:128] + pltpu.roll(high[:128], 64, 1)
    second = pltpu.roll(low[128:], 64, 1) + high[128:]
    both = jnp.where(wide < 64, first, second)
    kvs[...] = pltpu.roll(both, quarter * 32, 1).astype(BF16)

    def k_copy(i):
        return remote(
            kvs, kvr.at[quarter], ksem_s.at[i], ksem_r.at[quarter], kv_head * 4 + lax.rem(quarter + i, 4), r
        )

    @pl.loop(1, 4)
    def _(i):
        k_copy(i).start()

    kvr[quarter] = kvs[...]

    @pl.loop(1, 4)
    def _(i):
        other = lax.rem(quarter + i, 4)
        remote(kvs, kvr.at[other], ksem_s.at[i], ksem_r.at[other], kv_head * 4 + other, r).wait_recv()

    block = lax.div(wide, 32)
    for turn in range(4):
        merged = kvr[(3 - turn) % 4].astype(F32)
        for j in range(4):
            if (j + turn) % 4 != 3:
                merged = jnp.where(block == (j + turn) % 4, kvr[j].astype(F32), merged)
        if turn:
            merged = pltpu.roll(merged, 128 - 32 * turn, 1)
        dest = values_all if turn % 2 else keys_all
        dest[(turn // 2) * 128 : (turn // 2) * 128 + 128, :] = merged.astype(BF16)

    token = lax.broadcasted_iota(jnp.int32, (64, 256), 0)
    position = lax.div(token, 16) * 64 + lax.rem(token, 16) + served * 16
    key_pos = lax.broadcasted_iota(jnp.int32, (64, 256), 1)
    length = len_ref[0]
    allowed = jnp.logical_and(key_pos <= position, key_pos < length)
    live = position[:, :128] < length
    for h in range(GROUP):
        scores = lax.dot_general(
            qall[:, h * 128 : h * 128 + 128], keys_all[...], (((1,), (1,)), ((), ())), preferred_element_type=F32
        )
        scores = jnp.where(allowed, scores * HEAD ** (-0.5), -jnp.inf)
        expo = jnp.exp(scores - jnp.max(scores, axis=1, keepdims=True))
        probs = (expo / jnp.sum(expo, axis=1, keepdims=True)).astype(BF16)
        mixed = jnp.dot(probs, values_all[...], preferred_element_type=F32)
        mixed = jnp.where(live, mixed, 0.0).astype(BF16)
        for m in range(4):
            cs[m, :, h * 128 : h * 128 + 128] = mixed[m * 16 : m * 16 + 16]

    def c_copy(i):
        other = lax.rem(kv_head + 2 + i, 4)
        return remote(cs.at[other], cr.at[kv_head], csem_s.at[i], csem_r.at[kv_head], other * 4 + served, r)

    @pl.loop(0, 4)
    def _(i):
        c_copy(i).start()

    @pl.loop(0, 4)
    def _(i):
        remote(cs.at[i], cr.at[i], csem_s.at[i], csem_r.at[i], i * 4 + served, r).wait_recv()

    for m in range(4):
        ctx_ref[:, m * 640 : m * 640 + 640] = cr[m].astype(F32)

    for copy in a_copies:
        copy.wait_send()

    @pl.loop(0, 4)
    def _(i):
        c_copy(i).wait_send()

    @pl.loop(1, 4)
    def _(i):
        q_copy(i).wait_send()
        k_copy(i).wait_send()

    @pl.loop(0, 15)
    def _(i):
        z_copy(i).wait_send()
        gx_copy(i, zdev(came(i))).wait_send()
        gm_copy(i, zdev(came(i))).wait_send()

    for i in range(7):
        gz_copy(i).wait_send()
    for i in (4, 5):
        for turn in range(4):
            gr_copy(i, turn, zdev(came(i))).wait_send()
    gx_copy(15, r).wait_send()
    gm_copy(31, r).wait_send()

    @pl.loop(0, 16)
    def _(i):
        gm_copy(15 + i, xslot(i)).wait_send()
        x_copy(i).wait_send()

        @pl.when(jnp.logical_not(s_here(i)))
        def _():
            s_copy(i).wait_send()


def update(gradients, tokens, query_weight_t, master, first, second, lengths):
    vm = pltpu.VMEM
    dma = pltpu.SemaphoreType.DMA
    state = jax.ShapeDtypeStruct((80, 1, 64), F32)
    anyspace = pl.BlockSpec(memory_space=pl.ANY)
    vmem = pl.BlockSpec(memory_space=pltpu.VMEM)
    return pl.pallas_call(
        update_kernel,
        out_shape=(
            state, state, state,
            jax.ShapeDtypeStruct((16, QCOLS), F32),
        ),
        in_specs=[anyspace] * 6 + [pl.BlockSpec(memory_space=pltpu.SMEM)],
        out_specs=(vmem,) * 4,
        scratch_shapes=[
            vm((320, 1024), BF16),
            vm((256, 5120), BF16),
            vm((160, 5120), BF16),
            vm((80, 1, 64), F32), vm((80, 1, 64), F32), vm((80, 1, 64), F32),
            vm((320, 512), BF16),
            vm((640, 128), F32),
            vm((16, 5, 8, 128), BF16),
            vm((16, 5, 8, 128), BF16),
            vm((640, 128), F32),
            vm((16, 5, 8, 128), BF16),
            vm((16, 5, 8, 128), BF16),
            vm((64, 128), F32),
            vm((16, 8, 128), F32),
            vm((16, 8, 128), F32),
            vm((64, 128), F32),
            vm((64, 5, 8, 128), BF16),
            vm((2560, 128), F32),
            vm((2560, 128), BF16),
            vm((4, 64, 256), BF16),
            vm((4, 64, 256), BF16),
            vm((64, 640), BF16),
            vm((128, 128), BF16),
            vm((4, 128, 128), BF16),
            vm((256, 128), BF16),
            vm((256, 128), BF16),
            vm((4, 16, 640), BF16),
            vm((4, 16, 640), BF16),
            dma((6,)), dma((4,)), dma((4,)), dma((16,)), dma((16,)), dma((15,)), dma((16,)),
            dma((16,)), dma((16,)), dma((7,)), dma((8,)), dma((16,)), dma((32,)), dma((64,)),
            dma((4,)), dma((4,)), dma((4,)), dma((4,)), dma((4,)), dma((4,)),
        ],
        compiler_params=pltpu.CompilerParams(collective_id=0, has_side_effects=True),
        name="update",
    )(gradients, tokens, query_weight_t, master, first, second, lengths)


def finish_kernel(*refs):
    sources, targets, held, came, left = refs[:4], refs[4:8], refs[8:12], refs[12], refs[13]
    for i in range(4):
        pltpu.make_async_copy(sources[i], held[i], came.at[i]).start()
    for i in range(4):
        pltpu.make_async_copy(sources[i], held[i], came.at[i]).wait()
        pltpu.make_async_copy(held[i], targets[i], left.at[i]).start()
    for i in range(4):
        pltpu.make_async_copy(held[i], targets[i], left.at[i]).wait()


def finish(arrays):
    anyspace = pl.BlockSpec(memory_space=pl.ANY)
    return pl.pallas_call(
        finish_kernel,
        out_shape=[jax.ShapeDtypeStruct(a.shape, a.dtype) for a in arrays],
        in_specs=[anyspace] * 4,
        out_specs=[anyspace] * 4,
        scratch_shapes=[pltpu.VMEM(a.shape, a.dtype) for a in arrays] + [pltpu.SemaphoreType.DMA((4,))] * 2,
        name="finish",
    )(*arrays)


def on_device(gradients, hidden, lengths, query_weight, master, first_moment, second_moment):
    states = [a.reshape(80, 1, 64) for a in (master, first_moment, second_moment)]
    *states, context = finish(update(gradients[0], hidden[0], query_weight.T, *states, lengths))
    return (*[a.reshape(16, 1, 5, 64) for a in states], context[None])


def solution(mesh):
    in_specs = (
        P("replica", "section", None),
        P("replica", None, None),
        P("replica"),
        P(None, "section"),
        P(None, "replica", None, "section"),
        P(None, "replica", None, "section"),
        P(None, "replica", None, "section"),
    )
    out_specs = (
        P(None, "replica", None, "section"),
        P(None, "replica", None, "section"),
        P(None, "replica", None, "section"),
        P("replica", "section", None),
    )
    return jax.shard_map(
        on_device, mesh=mesh, in_specs=in_specs, out_specs=out_specs, check_vma=False
    )
```

```python
import functools

import jax
import jax.numpy as jnp
from jax import lax
from jax.experimental import pallas as pl
from jax.experimental.pallas import tpu as pltpu
from jax.sharding import PartitionSpec as P

HEAD = 128
GROUP = 5
QCOLS = 2560
F32 = jnp.float32
BF16 = jnp.bfloat16
MESH = pl.DeviceIdType.MESH

BETA_ONE = 0.9
BETA_TWO = 0.95
EPSILON = 1e-08
DECAY = 0.1
RATE = 0.001
CORRECT_ONE = 1.0 - 0.9**50
CORRECT_TWO = 1.0 - 0.95**50


def adam_step(gradient, weight, first_moment, second_moment):
    new_first = BETA_ONE * first_moment + (1.0 - BETA_ONE) * gradient
    new_second = BETA_TWO * second_moment + (1.0 - BETA_TWO) * gradient * gradient
    direction = new_first / CORRECT_ONE / (jnp.sqrt(new_second / CORRECT_TWO) + EPSILON)
    new_master = weight - RATE * (direction + DECAY * weight)
    return (new_master, new_first, new_second)


def far_first(i):
    half = lax.div(i + 1, 2)
    return 8 + half * (1 - 2 * lax.rem(i, 2))


def near_first(i):
    return far_first(14 - i)


def update_kernel(
    g_hbm, hid_hbm, qw_hbm, ma_hbm, fm_hbm, sm_hbm, len_ref,
    nm_ref, nf_ref, ns_ref, ctx_ref,
    gv, hv, qv, ma, fm, sm, ra, xo32, xs, xr, z32, zs, rz, sz, ss, rs, m2, agb, w2, w2b,
    qs, qr, qall, kvs, kvr, keys_all, values_all, cs, cr,
    lsem, asem_s, asem_r, xsem_s, xsem_r, zsem_s, zsem_r, ssem_s, ssem_r, gz_s, gr_s, gx_s, gm_s, g_r,
    qsem_s, qsem_r, ksem_s, ksem_r, csem_s, csem_r,
):
    p = lax.axis_index("section")
    r = lax.axis_index("replica")
    core = lax.rem(r, 2)
    z = lax.rem(lax.div(r, 2), 16)
    xh = lax.div(r, 32)
    own_core = lax.div(p, 8)
    mate = r + 1 - 2 * core
    xmate = r + 32 - 64 * xh
    has_self = jnp.where(own_core == core, 1, 0)
    kv_head = lax.div(p, 4)
    quarter = lax.rem(p, 4)
    served = lax.rem(p + 2, 4)

    def zdev(zz):
        return xh * 32 + zz * 2 + core

    local = [
        pltpu.make_async_copy(src, dst, lsem.at[i])
        for i, (src, dst) in enumerate(
            ((g_hbm, gv), (hid_hbm, hv), (qw_hbm, qv), (ma_hbm, ma), (fm_hbm, fm), (sm_hbm, sm))
        )
    ]
    for copy in local:
        copy.start()

    barrier = pltpu.get_barrier_semaphore()

    def greet(section, replica):
        pl.semaphore_signal(
            barrier, inc=1, device_id={"section": section, "replica": replica}, device_id_type=MESH
        )

    greet(p, mate)
    greet(p, xmate)

    @pl.loop(0, 15)
    def _(i):
        greet(p, zdev(lax.rem(z + far_first(i), 16)))

    @pl.loop(0, 16)
    def _(i):
        @pl.when(jnp.logical_not(jnp.logical_and(i == p, own_core == core)))
        def _():
            greet(i, r - core + own_core)

    @pl.loop(1, 4)
    def _(i):
        greet(kv_head * 4 + lax.rem(quarter + i, 4), r)

    @pl.loop(0, 4)
    def _(i):
        greet(i * 4 + served, r)

    local[0].wait()
    pl.semaphore_wait(barrier, 40 - has_self)

    def remote(src, dst, send, recv, section, replica):
        return pltpu.make_async_remote_copy(
            src_ref=src, dst_ref=dst, send_sem=send, recv_sem=recv,
            device_id={"section": section, "replica": replica}, device_id_type=MESH,
        )

    theirs = pl.multiple_of((1 - core) * 256, 256)
    mine = pl.multiple_of(core * 256, 256)
    a_copies = [
        remote(gv.at[pl.ds(row, 160), pl.ds(pl.multiple_of(theirs + side * 512, 256), 256)],
               ra.at[pl.ds(row, 160), pl.ds(side * 256, 256)],
               asem_s.at[turn * 2 + side], asem_r.at[turn * 2 + side], p, mate)
        for turn, row in enumerate((pl.multiple_of((1 - xh) * 160, 16), pl.multiple_of(xh * 160, 16)))
        for side in range(2)
    ]
    for copy in a_copies:
        copy.start()

    def paired(half, out):
        @pl.loop(0, 10)
        def _(ch):
            row = pl.multiple_of(half * 160 + ch * 16, 16)
            for side in range(2):
                own = gv[pl.ds(row, 16), pl.ds(pl.multiple_of(mine + side * 512, 256), 256)]
                total = own.astype(F32) + ra[pl.ds(row, 16), side * 256 : side * 256 + 256].astype(F32)
                for eight in range(2):
                    for tile in range(2):
                        out[pl.ds(ch * 64 + eight * 32 + side * 2 + tile, 8, stride=4), :] = total[
                            eight * 8 : eight * 8 + 8, tile * 128 : tile * 128 + 128
                        ]

    def place(i):
        return lax.rem(z + far_first(i), 16)

    def rows_of(ref, zz):
        return ref[pl.ds(pl.multiple_of(zz * 40, 8), 40), :]

    def x_copy(i):
        return remote(xs.at[place(i)], xr.at[place(i)], xsem_s.at[i], xsem_r.at[place(i)], p, xmate)

    a_copies[0].wait_recv()
    a_copies[1].wait_recv()
    paired(1 - xh, xo32)

    @pl.loop(0, 16)
    def _(i):
        xs[place(i)] = rows_of(xo32, place(i)).astype(BF16).reshape(5, 8, 128)
        x_copy(i).start()

    a_copies[2].wait_recv()
    a_copies[3].wait_recv()
    paired(xh, z32)

    def z_copy(i):
        return remote(zs.at[place(i)], rz.at[z], zsem_s.at[i], zsem_r.at[z], p, zdev(place(i)))

    @pl.loop(0, 15)
    def _(i):
        x_copy(i).wait_recv()
        piece = rows_of(z32, place(i)) + xr[place(i)].astype(F32).reshape(40, 128)
        zs[place(i)] = piece.astype(BF16).reshape(5, 8, 128)
        z_copy(i).start()

    x_copy(15).wait_recv()
    sz[0:40, :] = rows_of(z32, z) + xr[z].astype(F32).reshape(40, 128)
    sz[40:64, :] = jnp.zeros((24, 128), F32)

    local[1].wait()
    local[2].wait()
    queries = lax.dot_general(hv[...], qv[...], (((1,), (1,)), ((), ())), preferred_element_type=F32)
    queries = queries.astype(BF16)
    for j in range(4):
        for m in range(4):
            qs[j, m * 16 : m * 16 + 16, 0:160] = queries[m * 64 + j * 16 : m * 64 + j * 16 + 16]

    def q_copy(i):
        other = lax.rem(quarter + i, 4)
        return remote(
            qs.at[lax.rem(other + 2, 4)], qr.at[quarter], qsem_s.at[i], qsem_r.at[quarter], kv_head * 4 + other, r
        )

    @pl.loop(1, 4)
    def _(i):
        q_copy(i).start()

    qr[quarter] = qs[served]

    @pl.loop(0, 15)
    def _(i):
        other = lax.rem(z + near_first(i), 16)
        remote(zs.at[other], rz.at[other], zsem_s.at[i], zsem_r.at[other], p, zdev(other)).wait_recv()
        sz[0:40, :] += rz[other].astype(F32).reshape(40, 128)

    lane = lax.broadcasted_iota(jnp.int32, (8, 128), 1)
    for cc in range(2):
        for quad in range(2):
            keys = sz[pl.ds(cc * 20 + quad, 8, stride=4), :]
            values = sz[pl.ds(cc * 20 + 2 + quad, 8, stride=4), :]
            for j in range(4):
                key_part = pltpu.roll(keys, (128 - 32 * j) % 128, 1) if j else keys
                value_part = pltpu.roll(values, (160 - 32 * j) % 128, 1) if j != 1 else values
                ss[cc * 8 + quad * 4 + j] = jnp.where(lane < 32, key_part, value_part)

    def s_copy(i):
        section = core * 8 + lax.rem(i, 8)
        return remote(ss.at[i], rs.at[p], ssem_s.at[i], ssem_r.at[p], section, r - core + lax.div(i, 8))

    def s_here(i):
        return jnp.logical_and(core * 8 + lax.rem(i, 8) == p, lax.div(i, 8) == core)

    @pl.loop(0, 16)
    def _(i):
        @pl.when(jnp.logical_not(s_here(i)))
        def _():
            s_copy(i).start()

    @pl.when(own_core == core)
    def _():
        rs[p] = ss[core * 8 + lax.rem(p, 8)]

    @pl.loop(1, 4)
    def _(i):
        other = lax.rem(quarter + i, 4)
        remote(qs.at[other], qr.at[other], qsem_s.at[i], qsem_r.at[other], kv_head * 4 + other, r).wait_recv()

    for j in range(4):
        qall[:, j * 160 : j * 160 + 160] = qr[j, :, 0:160]

    for copy in local[3:]:
        copy.wait()

    @pl.loop(0, 16)
    def _(i):
        @pl.when(jnp.logical_not(jnp.logical_and(i == p, own_core == core)))
        def _():
            remote(ss.at[i], rs.at[i], ssem_s.at[i], ssem_r.at[i], i, r - core + own_core).wait_recv()

    @pl.loop(0, 16)
    def _(i):
        rows = pl.ds(i * 5, 5)
        new_master, new_first, new_second = adam_step(
            rs[i, 0:5, 0:64], ma[rows, 0, :], fm[rows, 0, :], sm[rows, 0, :]
        )
        nm_ref[rows, 0, :] = new_master
        nf_ref[rows, 0, :] = new_first
        ns_ref[rows, 0, :] = new_second
        rs[i, 0:5, 0:64] = new_master

    for i in range(8):
        m2[i * 8 : i * 8 + 8, :] = jnp.where(lane < 64, rs[i], pltpu.roll(rs[i + 8], 64, 1))
    for k in range(5):
        agb[r, k] = m2[pl.ds(k, 8, stride=8), :].astype(BF16)

    def came(i):
        late = jnp.where(i == 6, 14, jnp.where(i < 11, i - 3, i - 1))
        index = jnp.where(i < 4, i, jnp.where(i < 6, i + 4, late))
        return lax.rem(z + near_first(index), 16)

    def gz_copy(i):
        away = (5, 11, 8, 1, 15, 2, 14)[i]
        return remote(agb.at[r], agb.at[r], gz_s.at[i], g_r.at[r], p, zdev(lax.rem(z + away, 16)))

    def gr_copy(at, turn, slot):
        to = zdev(lax.rem(z + (1, 15, 2, 14)[turn], 16))
        return remote(agb.at[slot], agb.at[slot], gr_s.at[at * 4 + turn], g_r.at[slot], p, to)

    def gx_copy(i, slot):
        return remote(agb.at[slot], agb.at[slot], gx_s.at[i], g_r.at[slot], p, xmate)

    def gm_copy(i, slot):
        return remote(agb.at[slot], agb.at[slot], gm_s.at[i], g_r.at[slot], p, mate)

    def arrive(slot):
        remote(agb.at[slot], agb.at[slot], gm_s.at[0], g_r.at[slot], p, mate).wait_recv()

    def scatter(slot):
        for k in range(5):
            w2[pl.ds(slot * 5 + k, 8, stride=320), :] = agb[slot, k].astype(F32)

    gx_copy(15, r).start()

    for i in range(7):
        gz_copy(i).start()
    gm_copy(31, r).start()
    scatter(r)

    def xslot(i):
        return (1 - xh) * 32 + jnp.where(i == 0, z, came(i - 1)) * 2 + core

    def from_mate(slot):
        arrive(slot + 1 - 2 * core)
        scatter(slot + 1 - 2 * core)

    def own_ring(i):
        return zdev(jnp.where(i == 0, z, came(i - 1)))

    @pl.loop(0, 7)
    def _(i):
        slot = zdev(came(i))
        arrive(slot)

        @pl.when(jnp.logical_and(i >= 4, i < 6))
        def _():
            for turn in range(4):
                gr_copy(i - 4, turn, slot).start()

        gx_copy(i, slot).start()
        gm_copy(i, slot).start()
        scatter(slot)

    @pl.loop(0, 8)
    def _(i):
        slot = xslot(i)
        arrive(slot)

        @pl.when(jnp.logical_and(i >= 5, i < 7))
        def _():
            for turn in range(4):
                gr_copy(i - 3, turn, slot).start()

        gm_copy(15 + i, slot).start()
        scatter(slot)
        from_mate(own_ring(i))

    @pl.loop(7, 15)
    def _(i):
        slot = zdev(came(i))
        arrive(slot)
        gm_copy(i, slot).start()
        scatter(slot)
        from_mate(xslot(i - 7))

    @pl.loop(8, 16)
    def _(i):
        slot = xslot(i)
        arrive(slot)
        gm_copy(15 + i, slot).start()
        scatter(slot)
        from_mate(own_ring(i))

    @pl.loop(8, 16)
    def _(i):
        from_mate(xslot(i))

    w2b[...] = w2[...].astype(BF16)
    low = jnp.dot(hv[:, :2560], w2b[...], preferred_element_type=F32)
    high = jnp.dot(hv[:, 2560:], w2b[...], preferred_element_type=F32)
    wide = lax.broadcasted_iota(jnp.int32, (128, 128), 1)
    first = low[:128] + pltpu.roll(high[:128], 64, 1)
    second = pltpu.roll(low[128:], 64, 1) + high[128:]
    both = jnp.where(wide < 64, first, second)
    kvs[...] = pltpu.roll(both, quarter * 32, 1).astype(BF16)

    def k_copy(i):
        return remote(
            kvs, kvr.at[quarter], ksem_s.at[i], ksem_r.at[quarter], kv_head * 4 + lax.rem(quarter + i, 4), r
        )

    @pl.loop(1, 4)
    def _(i):
        k_copy(i).start()

    kvr[quarter] = kvs[...]

    @pl.loop(1, 4)
    def _(i):
        other = lax.rem(quarter + i, 4)
        remote(kvs, kvr.at[other], ksem_s.at[i], ksem_r.at[other], kv_head * 4 + other, r).wait_recv()

    block = lax.div(wide, 32)
    for turn in range(4):
        merged = kvr[(3 - turn) % 4].astype(F32)
        for j in range(4):
            if (j + turn) % 4 != 3:
                merged = jnp.where(block == (j + turn) % 4, kvr[j].astype(F32), merged)
        if turn:
            merged = pltpu.roll(merged, 128 - 32 * turn, 1)
        dest = values_all if turn % 2 else keys_all
        dest[(turn // 2) * 128 : (turn // 2) * 128 + 128, :] = merged.astype(BF16)

    token = lax.broadcasted_iota(jnp.int32, (64, 256), 0)
    position = lax.div(token, 16) * 64 + lax.rem(token, 16) + served * 16
    key_pos = lax.broadcasted_iota(jnp.int32, (64, 256), 1)
    length = len_ref[0]
    allowed = jnp.logical_and(key_pos <= position, key_pos < length)
    live = position[:, :128] < length
    for h in range(GROUP):
        scores = lax.dot_general(
            qall[:, h * 128 : h * 128 + 128], keys_all[...], (((1,), (1,)), ((), ())), preferred_element_type=F32
        )
        scores = jnp.where(allowed, scores * HEAD ** (-0.5), -jnp.inf)
        expo = jnp.exp(scores - jnp.max(scores, axis=1, keepdims=True))
        probs = (expo / jnp.sum(expo, axis=1, keepdims=True)).astype(BF16)
        mixed = jnp.dot(probs, values_all[...], preferred_element_type=F32)
        mixed = jnp.where(live, mixed, 0.0).astype(BF16)
        for m in range(4):
            cs[m, :, h * 128 : h * 128 + 128] = mixed[m * 16 : m * 16 + 16]

    def c_copy(i):
        other = lax.rem(kv_head + 2 + i, 4)
        return remote(cs.at[other], cr.at[kv_head], csem_s.at[i], csem_r.at[kv_head], other * 4 + served, r)

    @pl.loop(0, 4)
    def _(i):
        c_copy(i).start()

    @pl.loop(0, 4)
    def _(i):
        remote(cs.at[i], cr.at[i], csem_s.at[i], csem_r.at[i], i * 4 + served, r).wait_recv()

    for m in range(4):
        ctx_ref[:, m * 640 : m * 640 + 640] = cr[m].astype(F32)

    for copy in a_copies:
        copy.wait_send()

    @pl.loop(0, 4)
    def _(i):
        c_copy(i).wait_send()

    @pl.loop(1, 4)
    def _(i):
        q_copy(i).wait_send()
        k_copy(i).wait_send()

    @pl.loop(0, 15)
    def _(i):
        z_copy(i).wait_send()
        gm_copy(i, zdev(came(i))).wait_send()

    for i in range(7):
        gz_copy(i).wait_send()
        gx_copy(i, zdev(came(i))).wait_send()
    for at in range(2):
        for turn in range(4):
            gr_copy(at, turn, zdev(came(at + 4))).wait_send()
            gr_copy(at + 2, turn, xslot(at + 5)).wait_send()
    gx_copy(15, r).wait_send()
    gm_copy(31, r).wait_send()

    @pl.loop(0, 16)
    def _(i):
        gm_copy(15 + i, xslot(i)).wait_send()
        x_copy(i).wait_send()

        @pl.when(jnp.logical_not(s_here(i)))
        def _():
            s_copy(i).wait_send()


def update(gradients, tokens, query_weight_t, master, first, second, lengths):
    vm = pltpu.VMEM
    dma = pltpu.SemaphoreType.DMA
    state = jax.ShapeDtypeStruct((80, 1, 64), F32)
    anyspace = pl.BlockSpec(memory_space=pl.ANY)
    vmem = pl.BlockSpec(memory_space=pltpu.VMEM)
    return pl.pallas_call(
        update_kernel,
        out_shape=(
            state, state, state,
            jax.ShapeDtypeStruct((16, QCOLS), F32),
        ),
        in_specs=[anyspace] * 6 + [pl.BlockSpec(memory_space=pltpu.SMEM)],
        out_specs=(vmem,) * 4,
        scratch_shapes=[
            vm((320, 1024), BF16),
            vm((256, 5120), BF16),
            vm((160, 5120), BF16),
            vm((80, 1, 64), F32), vm((80, 1, 64), F32), vm((80, 1, 64), F32),
            vm((320, 512), BF16),
            vm((640, 128), F32),
            vm((16, 5, 8, 128), BF16),
            vm((16, 5, 8, 128), BF16),
            vm((640, 128), F32),
            vm((16, 5, 8, 128), BF16),
            vm((16, 5, 8, 128), BF16),
            vm((64, 128), F32),
            vm((16, 8, 128), F32),
            vm((16, 8, 128), F32),
            vm((64, 128), F32),
            vm((64, 5, 8, 128), BF16),
            vm((2560, 128), F32),
            vm((2560, 128), BF16),
            vm((4, 64, 256), BF16),
            vm((4, 64, 256), BF16),
            vm((64, 640), BF16),
            vm((128, 128), BF16),
            vm((4, 128, 128), BF16),
            vm((256, 128), BF16),
            vm((256, 128), BF16),
            vm((4, 16, 640), BF16),
            vm((4, 16, 640), BF16),
            dma((6,)), dma((4,)), dma((4,)), dma((16,)), dma((16,)), dma((15,)), dma((16,)),
            dma((16,)), dma((16,)), dma((7,)), dma((16,)), dma((16,)), dma((32,)), dma((64,)),
            dma((4,)), dma((4,)), dma((4,)), dma((4,)), dma((4,)), dma((4,)),
        ],
        compiler_params=pltpu.CompilerParams(collective_id=0, has_side_effects=True),
        name="update",
    )(gradients, tokens, query_weight_t, master, first, second, lengths)


def finish_kernel(*refs):
    sources, targets, held, came, left = refs[:4], refs[4:8], refs[8:12], refs[12], refs[13]
    for i in range(4):
        pltpu.make_async_copy(sources[i], held[i], came.at[i]).start()
    for i in range(4):
        pltpu.make_async_copy(sources[i], held[i], came.at[i]).wait()
        pltpu.make_async_copy(held[i], targets[i], left.at[i]).start()
    for i in range(4):
        pltpu.make_async_copy(held[i], targets[i], left.at[i]).wait()


def finish(arrays):
    anyspace = pl.BlockSpec(memory_space=pl.ANY)
    return pl.pallas_call(
        finish_kernel,
        out_shape=[jax.ShapeDtypeStruct(a.shape, a.dtype) for a in arrays],
        in_specs=[anyspace] * 4,
        out_specs=[anyspace] * 4,
        scratch_shapes=[pltpu.VMEM(a.shape, a.dtype) for a in arrays] + [pltpu.SemaphoreType.DMA((4,))] * 2,
        name="finish",
    )(*arrays)


def on_device(gradients, hidden, lengths, query_weight, master, first_moment, second_moment):
    states = [a.reshape(80, 1, 64) for a in (master, first_moment, second_moment)]
    *states, context = finish(update(gradients[0], hidden[0], query_weight.T, *states, lengths))
    return (*[a.reshape(16, 1, 5, 64) for a in states], context[None])


def solution(mesh):
    in_specs = (
        P("replica", "section", None),
        P("replica", None, None),
        P("replica"),
        P(None, "section"),
        P(None, "replica", None, "section"),
        P(None, "replica", None, "section"),
        P(None, "replica", None, "section"),
    )
    out_specs = (
        P(None, "replica", None, "section"),
        P(None, "replica", None, "section"),
        P(None, "replica", None, "section"),
        P("replica", "section", None),
    )
    return jax.shard_map(
        on_device, mesh=mesh, in_specs=in_specs, out_specs=out_specs, check_vma=False
    )
```

```python
import functools

import jax
import jax.numpy as jnp
from jax import lax
from jax.experimental import pallas as pl
from jax.experimental.pallas import tpu as pltpu
from jax.sharding import PartitionSpec as P

HEAD = 128
GROUP = 5
QCOLS = 2560
F32 = jnp.float32
BF16 = jnp.bfloat16
MESH = pl.DeviceIdType.MESH

BETA_ONE = 0.9
BETA_TWO = 0.95
EPSILON = 1e-08
DECAY = 0.1
RATE = 0.001
CORRECT_ONE = 1.0 - 0.9**50
CORRECT_TWO = 1.0 - 0.95**50


def adam_step(gradient, weight, first_moment, second_moment):
    new_first = BETA_ONE * first_moment + (1.0 - BETA_ONE) * gradient
    new_second = BETA_TWO * second_moment + (1.0 - BETA_TWO) * gradient * gradient
    direction = new_first / CORRECT_ONE / (jnp.sqrt(new_second / CORRECT_TWO) + EPSILON)
    new_master = weight - RATE * (direction + DECAY * weight)
    return (new_master, new_first, new_second)


def far_first(i):
    half = lax.div(i + 1, 2)
    return 8 + half * (1 - 2 * lax.rem(i, 2))


def near_first(i):
    return far_first(14 - i)


def update_kernel(
    g_hbm, hid_hbm, qw_hbm, ma_hbm, fm_hbm, sm_hbm, len_ref,
    nm_ref, nf_ref, ns_ref, ctx_ref,
    gv, hv, qv, ma, fm, sm, ra, xo32, xs, xr, z32, zs, rz, sz, ss, rs, m2, agb, w2, w2b,
    qs, qr, qall, kvs, kvr, keys_all, values_all, cs, cr,
    lsem, asem_s, asem_r, xsem_s, xsem_r, zsem_s, zsem_r, ssem_s, ssem_r, gz_s, gr_s, gx_s, gm_s, g_r,
    qsem_s, qsem_r, ksem_s, ksem_r, csem_s, csem_r,
):
    p = lax.axis_index("section")
    r = lax.axis_index("replica")
    core = lax.rem(r, 2)
    z = lax.rem(lax.div(r, 2), 16)
    xh = lax.div(r, 32)
    own_core = lax.div(p, 8)
    mate = r + 1 - 2 * core
    xmate = r + 32 - 64 * xh
    has_self = jnp.where(own_core == core, 1, 0)
    kv_head = lax.div(p, 4)
    quarter = lax.rem(p, 4)
    served = lax.rem(p + 2, 4)

    def zdev(zz):
        return xh * 32 + zz * 2 + core

    local = [
        pltpu.make_async_copy(src, dst, lsem.at[i])
        for i, (src, dst) in enumerate(
            ((g_hbm, gv), (hid_hbm, hv), (qw_hbm, qv), (ma_hbm, ma), (fm_hbm, fm), (sm_hbm, sm))
        )
    ]
    for copy in local:
        copy.start()

    barrier = pltpu.get_barrier_semaphore()

    def greet(section, replica):
        pl.semaphore_signal(
            barrier, inc=1, device_id={"section": section, "replica": replica}, device_id_type=MESH
        )

    greet(p, mate)
    greet(p, xmate)

    @pl.loop(0, 15)
    def _(i):
        greet(p, zdev(lax.rem(z + far_first(i), 16)))

    @pl.loop(0, 16)
    def _(i):
        @pl.when(jnp.logical_not(jnp.logical_and(i == p, own_core == core)))
        def _():
            greet(i, r - core + own_core)

    @pl.loop(1, 4)
    def _(i):
        greet(kv_head * 4 + lax.rem(quarter + i, 4), r)

    @pl.loop(0, 4)
    def _(i):
        greet(i * 4 + served, r)

    local[0].wait()
    pl.semaphore_wait(barrier, 40 - has_self)

    def remote(src, dst, send, recv, section, replica):
        return pltpu.make_async_remote_copy(
            src_ref=src, dst_ref=dst, send_sem=send, recv_sem=recv,
            device_id={"section": section, "replica": replica}, device_id_type=MESH,
        )

    theirs = pl.multiple_of((1 - core) * 256, 256)
    mine = pl.multiple_of(core * 256, 256)
    a_copies = [
        remote(gv.at[pl.ds(row, 160), pl.ds(pl.multiple_of(theirs + side * 512, 256), 256)],
               ra.at[pl.ds(row, 160), pl.ds(side * 256, 256)],
               asem_s.at[turn * 2 + side], asem_r.at[turn * 2 + side], p, mate)
        for turn, row in enumerate((pl.multiple_of((1 - xh) * 160, 16), pl.multiple_of(xh * 160, 16)))
        for side in range(2)
    ]
    for copy in a_copies:
        copy.start()

    def paired(half, out):
        @pl.loop(0, 10)
        def _(ch):
            row = pl.multiple_of(half * 160 + ch * 16, 16)
            for side in range(2):
                own = gv[pl.ds(row, 16), pl.ds(pl.multiple_of(mine + side * 512, 256), 256)]
                total = own.astype(F32) + ra[pl.ds(row, 16), side * 256 : side * 256 + 256].astype(F32)
                for eight in range(2):
                    for tile in range(2):
                        out[pl.ds(ch * 64 + eight * 32 + side * 2 + tile, 8, stride=4), :] = total[
                            eight * 8 : eight * 8 + 8, tile * 128 : tile * 128 + 128
                        ]

    def place(i):
        return lax.rem(z + far_first(i), 16)

    def rows_of(ref, zz):
        return ref[pl.ds(pl.multiple_of(zz * 40, 8), 40), :]

    def x_copy(i):
        return remote(xs.at[place(i)], xr.at[place(i)], xsem_s.at[i], xsem_r.at[place(i)], p, xmate)

    a_copies[0].wait_recv()
    a_copies[1].wait_recv()
    paired(1 - xh, xo32)

    @pl.loop(0, 16)
    def _(i):
        xs[place(i)] = rows_of(xo32, place(i)).astype(BF16).reshape(5, 8, 128)
        x_copy(i).start()

    a_copies[2].wait_recv()
    a_copies[3].wait_recv()
    paired(xh, z32)

    def z_copy(i):
        return remote(zs.at[place(i)], rz.at[z], zsem_s.at[i], zsem_r.at[z], p, zdev(place(i)))

    @pl.loop(0, 15)
    def _(i):
        x_copy(i).wait_recv()
        piece = rows_of(z32, place(i)) + xr[place(i)].astype(F32).reshape(40, 128)
        zs[place(i)] = piece.astype(BF16).reshape(5, 8, 128)
        z_copy(i).start()

    x_copy(15).wait_recv()
    sz[0:40, :] = rows_of(z32, z) + xr[z].astype(F32).reshape(40, 128)
    sz[40:64, :] = jnp.zeros((24, 128), F32)

    @pl.loop(0, 15)
    def _(i):
        other = lax.rem(z + near_first(i), 16)
        remote(zs.at[other], rz.at[other], zsem_s.at[i], zsem_r.at[other], p, zdev(other)).wait_recv()
        sz[0:40, :] += rz[other].astype(F32).reshape(40, 128)

    lane = lax.broadcasted_iota(jnp.int32, (8, 128), 1)
    for cc in range(2):
        for quad in range(2):
            keys = sz[pl.ds(cc * 20 + quad, 8, stride=4), :]
            values = sz[pl.ds(cc * 20 + 2 + quad, 8, stride=4), :]
            for j in range(4):
                key_part = pltpu.roll(keys, (128 - 32 * j) % 128, 1) if j else keys
                value_part = pltpu.roll(values, (160 - 32 * j) % 128, 1) if j != 1 else values
                ss[cc * 8 + quad * 4 + j] = jnp.where(lane < 32, key_part, value_part)

    def s_copy(i):
        section = core * 8 + lax.rem(i, 8)
        return remote(ss.at[i], rs.at[p], ssem_s.at[i], ssem_r.at[p], section, r - core + lax.div(i, 8))

    def s_here(i):
        return jnp.logical_and(core * 8 + lax.rem(i, 8) == p, lax.div(i, 8) == core)

    @pl.loop(0, 16)
    def _(i):
        @pl.when(jnp.logical_not(s_here(i)))
        def _():
            s_copy(i).start()

    @pl.when(own_core == core)
    def _():
        rs[p] = ss[core * 8 + lax.rem(p, 8)]

    local[1].wait()
    local[2].wait()
    queries = lax.dot_general(hv[...], qv[...], (((1,), (1,)), ((), ())), preferred_element_type=F32)
    queries = queries.astype(BF16)
    for j in range(4):
        for m in range(4):
            qs[j, m * 16 : m * 16 + 16, 0:160] = queries[m * 64 + j * 16 : m * 64 + j * 16 + 16]

    def q_copy(i):
        other = lax.rem(quarter + i, 4)
        return remote(
            qs.at[lax.rem(other + 2, 4)], qr.at[quarter], qsem_s.at[i], qsem_r.at[quarter], kv_head * 4 + other, r
        )

    @pl.loop(1, 4)
    def _(i):
        q_copy(i).start()

    qr[quarter] = qs[served]

    for copy in local[3:]:
        copy.wait()

    @pl.loop(0, 16)
    def _(i):
        @pl.when(jnp.logical_not(jnp.logical_and(i == p, own_core == core)))
        def _():
            remote(ss.at[i], rs.at[i], ssem_s.at[i], ssem_r.at[i], i, r - core + own_core).wait_recv()

    @pl.loop(0, 16)
    def _(i):
        rows = pl.ds(i * 5, 5)
        new_master, new_first, new_second = adam_step(
            rs[i, 0:5, 0:64], ma[rows, 0, :], fm[rows, 0, :], sm[rows, 0, :]
        )
        nm_ref[rows, 0, :] = new_master
        nf_ref[rows, 0, :] = new_first
        ns_ref[rows, 0, :] = new_second
        rs[i, 0:5, 0:64] = new_master

    for i in range(8):
        m2[i * 8 : i * 8 + 8, :] = jnp.where(lane < 64, rs[i], pltpu.roll(rs[i + 8], 64, 1))
    for k in range(5):
        agb[r, k] = m2[pl.ds(k, 8, stride=8), :].astype(BF16)

    def came(i):
        late = jnp.where(i == 6, 14, jnp.where(i < 11, i - 3, i - 1))
        index = jnp.where(i < 4, i, jnp.where(i < 6, i + 4, late))
        return lax.rem(z + near_first(index), 16)

    def gz_copy(i):
        away = (5, 11, 8, 1, 15, 2, 14)[i]
        return remote(agb.at[r], agb.at[r], gz_s.at[i], g_r.at[r], p, zdev(lax.rem(z + away, 16)))

    def gr_copy(at, turn, slot):
        to = zdev(lax.rem(z + (1, 15, 2, 14)[turn], 16))
        return remote(agb.at[slot], agb.at[slot], gr_s.at[at * 4 + turn], g_r.at[slot], p, to)

    def gx_copy(i, slot):
        return remote(agb.at[slot], agb.at[slot], gx_s.at[i], g_r.at[slot], p, xmate)

    def gm_copy(i, slot):
        return remote(agb.at[slot], agb.at[slot], gm_s.at[i], g_r.at[slot], p, mate)

    def arrive(slot):
        remote(agb.at[slot], agb.at[slot], gm_s.at[0], g_r.at[slot], p, mate).wait_recv()

    def scatter(slot):
        for k in range(5):
            w2[pl.ds(slot * 5 + k, 8, stride=320), :] = agb[slot, k].astype(F32)

    gx_copy(15, r).start()

    for i in range(7):
        gz_copy(i).start()
    gm_copy(31, r).start()
    scatter(r)

    @pl.loop(1, 4)
    def _(i):
        other = lax.rem(quarter + i, 4)
        remote(qs.at[other], qr.at[other], qsem_s.at[i], qsem_r.at[other], kv_head * 4 + other, r).wait_recv()

    for j in range(4):
        qall[:, j * 160 : j * 160 + 160] = qr[j, :, 0:160]

    def xslot(i):
        return (1 - xh) * 32 + jnp.where(i == 0, z, came(i - 1)) * 2 + core

    def from_mate(slot):
        arrive(slot + 1 - 2 * core)
        scatter(slot + 1 - 2 * core)

    def own_ring(i):
        return zdev(jnp.where(i == 0, z, came(i - 1)))

    @pl.loop(0, 7)
    def _(i):
        slot = zdev(came(i))
        arrive(slot)

        @pl.when(jnp.logical_and(i >= 4, i < 6))
        def _():
            for turn in range(4):
                gr_copy(i - 4, turn, slot).start()

        gx_copy(i, slot).start()
        gm_copy(i, slot).start()
        scatter(slot)

    @pl.loop(0, 8)
    def _(i):
        slot = xslot(i)
        arrive(slot)

        @pl.when(jnp.logical_and(i >= 5, i < 7))
        def _():
            for turn in range(4):
                gr_copy(i - 3, turn, slot).start()

        gm_copy(15 + i, slot).start()
        scatter(slot)
        from_mate(own_ring(i))

    @pl.loop(7, 15)
    def _(i):
        slot = zdev(came(i))
        arrive(slot)
        gm_copy(i, slot).start()
        scatter(slot)
        from_mate(xslot(i - 7))

    @pl.loop(8, 16)
    def _(i):
        slot = xslot(i)
        arrive(slot)
        gm_copy(15 + i, slot).start()
        scatter(slot)
        from_mate(own_ring(i))

    @pl.loop(8, 16)
    def _(i):
        from_mate(xslot(i))

    w2b[...] = w2[...].astype(BF16)
    low = jnp.dot(hv[:, :2560], w2b[...], preferred_element_type=F32)
    high = jnp.dot(hv[:, 2560:], w2b[...], preferred_element_type=F32)
    wide = lax.broadcasted_iota(jnp.int32, (128, 128), 1)
    first = low[:128] + pltpu.roll(high[:128], 64, 1)
    second = pltpu.roll(low[128:], 64, 1) + high[128:]
    both = jnp.where(wide < 64, first, second)
    kvs[...] = pltpu.roll(both, quarter * 32, 1).astype(BF16)

    def k_copy(i):
        return remote(kvs, kvr.at[quarter], ksem_s.at[i], ksem_r.at[quarter], kv_head * 4 + i, r)

    @pl.loop(0, 4)
    def _(i):
        far_end = jnp.where(quarter < 2, 3 - i, i)

        @pl.when(far_end != quarter)
        def _():
            k_copy(far_end).start()

    kvr[quarter] = kvs[...]

    @pl.loop(1, 4)
    def _(i):
        other = lax.rem(quarter + i, 4)
        remote(kvs, kvr.at[other], ksem_s.at[i], ksem_r.at[other], kv_head * 4 + other, r).wait_recv()

    block = lax.div(wide, 32)
    for turn in range(4):
        merged = kvr[(3 - turn) % 4].astype(F32)
        for j in range(4):
            if (j + turn) % 4 != 3:
                merged = jnp.where(block == (j + turn) % 4, kvr[j].astype(F32), merged)
        if turn:
            merged = pltpu.roll(merged, 128 - 32 * turn, 1)
        dest = values_all if turn % 2 else keys_all
        dest[(turn // 2) * 128 : (turn // 2) * 128 + 128, :] = merged.astype(BF16)

    token = lax.broadcasted_iota(jnp.int32, (64, 256), 0)
    position = lax.div(token, 16) * 64 + lax.rem(token, 16) + served * 16
    key_pos = lax.broadcasted_iota(jnp.int32, (64, 256), 1)
    length = len_ref[0]
    allowed = jnp.logical_and(key_pos <= position, key_pos < length)
    live = position[:, :128] < length
    for h in range(GROUP):
        scores = lax.dot_general(
            qall[:, h * 128 : h * 128 + 128], keys_all[...], (((1,), (1,)), ((), ())), preferred_element_type=F32
        )
        scores = jnp.where(allowed, scores * HEAD ** (-0.5), -jnp.inf)
        expo = jnp.exp(scores - jnp.max(scores, axis=1, keepdims=True))
        probs = (expo / jnp.sum(expo, axis=1, keepdims=True)).astype(BF16)
        mixed = jnp.dot(probs, values_all[...], preferred_element_type=F32)
        mixed = jnp.where(live, mixed, 0.0).astype(BF16)
        for m in range(4):
            cs[m, :, h * 128 : h * 128 + 128] = mixed[m * 16 : m * 16 + 16]

    def c_copy(i):
        other = lax.rem(kv_head + 2 + i, 4)
        return remote(cs.at[other], cr.at[kv_head], csem_s.at[i], csem_r.at[kv_head], other * 4 + served, r)

    @pl.loop(0, 4)
    def _(i):
        c_copy(i).start()

    @pl.loop(0, 4)
    def _(i):
        remote(cs.at[i], cr.at[i], csem_s.at[i], csem_r.at[i], i * 4 + served, r).wait_recv()

    for m in range(4):
        ctx_ref[:, m * 640 : m * 640 + 640] = cr[m].astype(F32)

    for copy in a_copies:
        copy.wait_send()

    @pl.loop(0, 4)
    def _(i):
        c_copy(i).wait_send()

    @pl.loop(1, 4)
    def _(i):
        q_copy(i).wait_send()
        k_copy(lax.rem(quarter + i, 4)).wait_send()

    @pl.loop(0, 15)
    def _(i):
        z_copy(i).wait_send()
        gm_copy(i, zdev(came(i))).wait_send()

    for i in range(7):
        gz_copy(i).wait_send()
        gx_copy(i, zdev(came(i))).wait_send()
    for at in range(2):
        for turn in range(4):
            gr_copy(at, turn, zdev(came(at + 4))).wait_send()
            gr_copy(at + 2, turn, xslot(at + 5)).wait_send()
    gx_copy(15, r).wait_send()
    gm_copy(31, r).wait_send()

    @pl.loop(0, 16)
    def _(i):
        gm_copy(15 + i, xslot(i)).wait_send()
        x_copy(i).wait_send()

        @pl.when(jnp.logical_not(s_here(i)))
        def _():
            s_copy(i).wait_send()


def update(gradients, tokens, query_weight_t, master, first, second, lengths):
    vm = pltpu.VMEM
    dma = pltpu.SemaphoreType.DMA
    state = jax.ShapeDtypeStruct((80, 1, 64), F32)
    anyspace = pl.BlockSpec(memory_space=pl.ANY)
    vmem = pl.BlockSpec(memory_space=pltpu.VMEM)
    return pl.pallas_call(
        update_kernel,
        out_shape=(
            state, state, state,
            jax.ShapeDtypeStruct((16, QCOLS), F32),
        ),
        in_specs=[anyspace] * 6 + [pl.BlockSpec(memory_space=pltpu.SMEM)],
        out_specs=(vmem,) * 4,
        scratch_shapes=[
            vm((320, 1024), BF16),
            vm((256, 5120), BF16),
            vm((160, 5120), BF16),
            vm((80, 1, 64), F32), vm((80, 1, 64), F32), vm((80, 1, 64), F32),
            vm((320, 512), BF16),
            vm((640, 128), F32),
            vm((16, 5, 8, 128), BF16),
            vm((16, 5, 8, 128), BF16),
            vm((640, 128), F32),
            vm((16, 5, 8, 128), BF16),
            vm((16, 5, 8, 128), BF16),
            vm((64, 128), F32),
            vm((16, 8, 128), F32),
            vm((16, 8, 128), F32),
            vm((64, 128), F32),
            vm((64, 5, 8, 128), BF16),
            vm((2560, 128), F32),
            vm((2560, 128), BF16),
            vm((4, 64, 256), BF16),
            vm((4, 64, 256), BF16),
            vm((64, 640), BF16),
            vm((128, 128), BF16),
            vm((4, 128, 128), BF16),
            vm((256, 128), BF16),
            vm((256, 128), BF16),
            vm((4, 16, 640), BF16),
            vm((4, 16, 640), BF16),
            dma((6,)), dma((4,)), dma((4,)), dma((16,)), dma((16,)), dma((15,)), dma((16,)),
            dma((16,)), dma((16,)), dma((7,)), dma((16,)), dma((16,)), dma((32,)), dma((64,)),
            dma((4,)), dma((4,)), dma((4,)), dma((4,)), dma((4,)), dma((4,)),
        ],
        compiler_params=pltpu.CompilerParams(collective_id=0, has_side_effects=True),
        name="update",
    )(gradients, tokens, query_weight_t, master, first, second, lengths)


def finish_kernel(*refs):
    sources, targets, held, came, left = refs[:4], refs[4:8], refs[8:12], refs[12], refs[13]
    for i in range(4):
        pltpu.make_async_copy(sources[i], held[i], came.at[i]).start()
    for i in range(4):
        pltpu.make_async_copy(sources[i], held[i], came.at[i]).wait()
        pltpu.make_async_copy(held[i], targets[i], left.at[i]).start()
    for i in range(4):
        pltpu.make_async_copy(held[i], targets[i], left.at[i]).wait()


def finish(arrays):
    anyspace = pl.BlockSpec(memory_space=pl.ANY)
    return pl.pallas_call(
        finish_kernel,
        out_shape=[jax.ShapeDtypeStruct(a.shape, a.dtype) for a in arrays],
        in_specs=[anyspace] * 4,
        out_specs=[anyspace] * 4,
        scratch_shapes=[pltpu.VMEM(a.shape, a.dtype) for a in arrays] + [pltpu.SemaphoreType.DMA((4,))] * 2,
        name="finish",
    )(*arrays)


def on_device(gradients, hidden, lengths, query_weight, master, first_moment, second_moment):
    states = [a.reshape(80, 1, 64) for a in (master, first_moment, second_moment)]
    *states, context = finish(update(gradients[0], hidden[0], query_weight.T, *states, lengths))
    return (*[a.reshape(16, 1, 5, 64) for a in states], context[None])


def solution(mesh):
    in_specs = (
        P("replica", "section", None),
        P("replica", None, None),
        P("replica"),
        P(None, "section"),
        P(None, "replica", None, "section"),
        P(None, "replica", None, "section"),
        P(None, "replica", None, "section"),
    )
    out_specs = (
        P(None, "replica", None, "section"),
        P(None, "replica", None, "section"),
        P(None, "replica", None, "section"),
        P("replica", "section", None),
    )
    return jax.shard_map(
        on_device, mesh=mesh, in_specs=in_specs, out_specs=out_specs, check_vma=False
    )
```
